32 devices in a mesh: gx: 2 (over y), gy: 4 (over z), gz: 4 (over x, core).
Axes of the slice: x: 2, y: 2, z: 4, core: 2. Of those that a mesh axis runs over, the one named last changes fastest.
Arguments:
- density: float32 [24, 64, 512], P('gx', 'gy', 'gz'), may hold values from 0.5 to 8
- potential: float32 [24, 64, 512], P('gx', 'gy', 'gz'), may hold values from -6 to 6
Outputs:
- corrected: float32 [24, 64, 512], P('gx', 'gy', 'gz')
The draws below stay inside these ranges and needn't reach their ends.
All inputs are finite; a program needn't handle non-finite values.
Results may differ from the reference program's by a relative error of at most 0.00005.
Values sent between devices are 32-bit elements; how exact they have to be, the bound alone decides.
A program may use at most 64 MiB of HBM per device.

```python
import math
import jax
import jax.numpy as jnp
from jax import lax

CX = 12
CY = 16
CZ = 128
SWEEPS = 2
NX = 24
NY = 64
NZ = 512
N_GX = 2
N_GY = 4
N_GZ = 4


def levels(stream_key, shape, split, low, top_value):
    factor_of = 1.0
    for dim, shards_of in split:
        steps = jax.random.uniform(jax.random.fold_in(jax.random.fold_in(stream_key, 6), dim), (shards_of,), jnp.float32, low / len(split), top_value / len(split))
        factor_of = factor_of * jnp.repeat(jnp.exp(steps), shape[dim] // shards_of).reshape((-1,) + (1,) * (len(shape) - 1 - dim))
    return factor_of


def normal_values(rng, shape, width, bound, split=(), kind=jnp.bfloat16):
    level = levels(rng, shape, split, -0.22, 0.18) if split else 1.0
    entries = jax.random.normal(rng, shape, jnp.float32) * width * level
    return jnp.minimum(jnp.maximum(entries, -bound), bound).astype(kind)


def setup_inputs(seed: int = 0) -> dict:
    splits = jax.random.split(jax.random.key(seed), 3)
    return {
        "density": jnp.clip(jnp.exp(math.log(8.0) - 2.7725887 * jax.random.uniform(splits[0], (NX, NY, NZ), jnp.float32) ** levels(splits[0], (NX, NY, NZ), ((0, 2), (1, 4), (2, 4)), -0.2, 0.2)), 0.5, 8.0),
        "potential": normal_values(splits[1], (NX, NY, NZ), 1.0, 6.0, ((0, 2), (1, 4), (2, 4)), jnp.float32),
    }


def beside_all(field):
    total = jnp.roll(field, -1, 0) + jnp.roll(field, 1, 0)
    total = total + jnp.roll(field, -1, 1) + jnp.roll(field, 1, 1)
    return total + jnp.roll(field, -1, 2) + jnp.roll(field, 1, 2)

def colour(shape, offset):
    summed = lax.broadcasted_iota(jnp.int32, shape, 0) + lax.broadcasted_iota(jnp.int32, shape, 1)
    summed = summed + lax.broadcasted_iota(jnp.int32, shape, 2) + offset
    return summed % 2 == 0

def smooth(field, source, red):
    field = jnp.where(red, (beside_all(field) - source) / 6.0, field)
    return jnp.where(red, field, (beside_all(field) - source) / 6.0)

def basis(count):
    rows = lax.broadcasted_iota(jnp.int32, (count, count), 0).astype(jnp.float32)
    cols = lax.broadcasted_iota(jnp.int32, (count, count), 1)
    freq = ((cols + 1) // 2).astype(jnp.float32)
    angle = 2.0 * jnp.pi * freq * rows / count
    full = jnp.sqrt(2.0 / count)
    single = 1.0 / jnp.sqrt(jnp.float32(count))
    top = 2 * ((cols + 1) // 2) == count
    table = jnp.where(cols % 2 == 1, jnp.cos(angle) * full, jnp.sin(angle) * full)
    table = jnp.where(top, jnp.cos(angle) * single, table)
    table = jnp.where(cols == 0, single, table)
    modes = ((jnp.arange(count, dtype=jnp.int32) + 1) // 2).astype(jnp.float32)
    return (table, 2.0 - 2.0 * jnp.cos(2.0 * jnp.pi * modes / count))

def coarse_solve(blocks, weight_x, weight_y, weight_z):
    nx, ny, nz = blocks.shape
    qx, lx = basis(nx)
    qy, ly = basis(ny)
    qz, lz = basis(nz)
    hi = lax.Precision.HIGHEST
    spectrum = jnp.einsum('ia,jb,kc,ijk->abc', qx, qy, qz, blocks, precision=hi)
    denom = weight_x * lx[:, None, None] + weight_y * ly[None, :, None] + weight_z * lz[None, None, :]
    zero = colour((nx, ny, nz), 0) & (lax.broadcasted_iota(jnp.int32, (nx, ny, nz), 0) + lax.broadcasted_iota(jnp.int32, (nx, ny, nz), 1) + lax.broadcasted_iota(jnp.int32, (nx, ny, nz), 2) == 0)
    safe = jnp.where(zero, jnp.float32(1.0), denom)
    spectrum = jnp.where(zero, jnp.float32(0.0), -spectrum / safe)
    return jnp.einsum('ia,jb,kc,abc->ijk', qx, qy, qz, spectrum, precision=hi)

def widen(field, bx, by, bz):
    return jnp.repeat(jnp.repeat(jnp.repeat(field, bx, 0), by, 1), bz, 2)

def reference(density, potential):
    source = density - jnp.sum(density) / (NX * NY * NZ)
    red = colour(source.shape, 0)
    fine = potential
    for sweep in range(SWEEPS):
        fine = smooth(fine, source, red)
    left = source - (beside_all(fine) - 6.0 * fine)
    level_one = left.reshape(NX // 2, 2, NY // 2, 2, NZ // 2, 2).sum(axis=(1, 3, 5)) * 0.5
    red_one = colour(level_one.shape, 0)
    error_one = jnp.zeros_like(level_one)
    for sweep in range(SWEEPS):
        error_one = smooth(error_one, level_one, red_one)
    rest = level_one - (beside_all(error_one) - 6.0 * error_one)
    bx, by, bz = (CX // 2, CY // 2, CZ // 2)
    blocks = rest.reshape(N_GX, bx, N_GY, by, N_GZ, bz).sum(axis=(1, 3, 5))
    coarse = coarse_solve(blocks, float(by * bz), float(bx * bz), float(bx * by))
    error_one = error_one + widen(coarse, bx, by, bz)
    for sweep in range(SWEEPS):
        error_one = smooth(error_one, level_one, red_one)
    fine = fine + widen(error_one, 2, 2, 2)
    for sweep in range(SWEEPS):
        fine = smooth(fine, source, red)
    return fine
```

```python
import functools
import numpy as np
import jax
import jax.numpy as jnp
from jax import lax
from jax.experimental import pallas as pl
from jax.experimental.pallas import tpu as pltpu
from jax.sharding import PartitionSpec as P

SWEEPS = 2
HI = lax.Precision.HIGHEST
MESH = pl.DeviceIdType.MESH
R = 8


def table(count):
    modes = (np.arange(count) + 1) // 2
    angle = 2 * np.pi * np.outer(np.arange(count), modes) / count
    q = np.where(np.arange(count) % 2 == 1, np.cos(angle), np.sin(angle)) * np.sqrt(2 / count)
    q = np.where(2 * modes == count, np.cos(angle) / np.sqrt(count), q)
    q[:, 0] = 1 / np.sqrt(count)
    return q, 2 - 2 * np.cos(2 * np.pi * modes / count)


def coarse_operator(nx, ny, nz, wx, wy, wz):
    qx, lx = table(nx)
    qy, ly = table(ny)
    qz, lz = table(nz)
    q = np.kron(np.kron(qx, qy), qz)
    lam = wx * lx[:, None, None] + wy * ly[None, :, None] + wz * lz[None, None, :]
    lam = lam.reshape(-1)
    inv = np.concatenate([[0.0], -1.0 / lam[1:]])
    return ((q * inv) @ q.T).astype(np.float32)


def kernel(
    dims, den_hbm, pot_hbm, op_hbm, out_ref, op_ref,
    own, pm, pa, pb, den, lv, ea, eb, e2, f2, gat, cv,
    pk_p, pk_l, pk_e, pk_f, rk_p, rk_l, rk_e, rk_f,
    ssem, rsem, gs, gr, lsem,
):
    nx, ny, nz, X, Y, Z = dims
    n = nx * ny * nz
    x1, y1, z1 = X // 2, Y // 2, Z // 2
    ix, iy, iz = lax.axis_index("gx"), lax.axis_index("gy"), lax.axis_index("gz")
    me = (ix * ny + iy) * nz + iz

    def around(i, count):
        return [i] + [jnp.where(i + o >= count, i + o - count, i + o) for o in range(1, count)]

    xs, ys, zs = around(ix, nx), around(iy, ny), around(iz, nz)

    def device(o):
        if isinstance(o, int):
            return (xs[o // (ny * nz)], ys[o // nz % ny], zs[o % nz])
        ox, oy, oz = o // (ny * nz), (o // nz) % ny, o % nz
        return (lax.rem(ix + ox, nx), lax.rem(iy + oy, ny), lax.rem(iz + oz, nz))

    def each_other(step):
        if n <= 64:
            for o in range(1, n):
                step(o, 0)
        else:
            lax.fori_loop(1, n, step, 0)

    load_p = pltpu.make_async_copy(pot_hbm, own, lsem.at[0])
    load_d = pltpu.make_async_copy(den_hbm, den.at[pl.ds(6, X), pl.ds(R, Y), pl.ds(0, Z)], lsem.at[1])
    load_p.start()
    load_d.start()
    load_op = pltpu.make_async_copy(op_hbm, op_ref, lsem.at[2])
    load_op.start()

    barrier = pltpu.get_barrier_semaphore()

    def greet(o, carry):
        pl.semaphore_signal(barrier, inc=1, device_id=device(o), device_id_type=MESH)
        return carry

    near = max(nx, ny, nz) <= 5
    steps = sorted({
        (dx % nx * ny + dy % ny) * nz + dz % nz
        for dx in (-1, 0, 1) for dy in (-1, 0, 1) for dz in (-1, 0, 1)
    } - {0})
    if near:
        for o in steps:
            greet(o, 0)
    else:
        each_other(greet)
    load_p.wait()
    load_d.wait()
    odd = (
        lax.broadcasted_iota(jnp.int32, (Y, Z), 0) + lax.broadcasted_iota(jnp.int32, (Y, Z), 1)
    ) % 2 == 1
    for j in range(X // 2):
        pm[3 + j, R : R + Y, 0:Z] = jnp.where(odd, own[2 * j], own[2 * j + 1])

    sems = iter(range(200))

    def pack(items, pk):
        base = 0
        sy = items[0][3][1]
        lane = lax.broadcasted_iota(jnp.int32, (sy, 128), 1)
        head = tail = jnp.zeros((sy, 128), jnp.float32)
        for buf, h, H, (sx, sy, sz), deep in items:
            for q in range(sx):
                v = buf[H + q, R : R + sy, 0:128]
                at = base + q * deep
                inside = (lane >= at) & (lane < at + deep)
                tail = jnp.where(inside, pltpu.roll(v, (at - (sz - deep)) % 128, 1), tail)
                head = jnp.where(inside, pltpu.roll(v, at, 1) if at else v, head)
            base += sx * deep
        assert base <= 128
        pk[0] = tail
        pk[1] = head

    def once(h, H, sx):
        return nx == 2 and 2 * h > sx and H >= sx

    def exchange(items, pk, rk):
        copies = []

        def send(src, dst, dx, dy, dz):
            k = next(sems)
            to = (xs[dx], ys[dy], zs[dz])
            copy = pltpu.make_async_remote_copy(
                src_ref=src, dst_ref=dst, send_sem=ssem.at[k], recv_sem=rsem.at[k],
                device_id=to, device_id_type=MESH,
            )
            copy.start()
            copies.append(copy)

        sy = items[0][3][1]
        rows_from = {0: pl.ds(R, sy), 1: pl.ds(sy, R), -1: pl.ds(R, R)}
        rows_to = {0: pl.ds(R, sy), 1: pl.ds(0, R), -1: pl.ds(R + sy, R)}
        for dx in (1, -1, 0):
            for dy in (1, -1, 0):
                for dz in (1, -1):
                    if dx == -1 and nx == 2:
                        continue
                    side = 0 if dz == 1 else 1
                    count = R if dy else sy
                    first = sy - R if dy == 1 else 0
                    send(
                        pk.at[side, pl.ds(first, count)],
                        rk.at[side, 1 - dx, 1 - dy, pl.ds(0, count)],
                        dx, dy, dz,
                    )
                if dx == 0 and dy == 0:
                    continue
                for buf, h, H, (sx, sy, sz), deep in items:
                    if once(h, H, sx):
                        if dx == -1:
                            continue
                        h = sx if dx else h
                    p_from = {0: pl.ds(H, sx), 1: pl.ds(H + sx - h, h), -1: pl.ds(H, h)}[dx]
                    p_to = {0: pl.ds(H, sx), 1: pl.ds(H - h, h), -1: pl.ds(H + sx, h)}[dx]
                    lanes = pl.ds(0, 128)
                    send(buf.at[p_from, rows_from[dy], lanes], buf.at[p_to, rows_to[dy], lanes], dx, dy, 0)
        return functools.partial(finish, items, rk, copies)

    def finish(items, rk, copies):
        for copy in copies:
            copy.wait()
        received = {}
        for group in range(3):
            slot = 0 if nx == 2 and group == 2 else group
            for side in range(2):
                received[side, group] = jnp.concatenate(
                    [rk[side, slot, 0, 0:R], rk[side, slot, 1], rk[side, slot, 2, 0:R]], axis=0
                )
        base = 0
        for buf, h, H, (sx, sy, sz), deep in items:
            rows = sy + 2 * R
            lane = lax.broadcasted_iota(jnp.int32, (rows, 128), 1)
            wide = sz == 128
            assert not (wide and once(h, H, sx))
            put = 0 if wide else sz
            for j in range(sx + 2 * h):
                group, q = (0, sx - h + j) if j < h else ((1, j - h) if j < h + sx else (2, j - h - sx))
                at = base + q * deep
                edge = jnp.where(
                    lane >= 112,
                    pltpu.roll(received[0, group], (128 - deep - at) % 128, 1),
                    pltpu.roll(received[1, group], (put - at) % 128, 1),
                )
                if wide:
                    buf[H - h + j, :, 128:256] = edge
                else:
                    at = H - sx + q if group == 2 and once(h, H, sx) else H - h + j
                    buf[H - h + j] = jnp.where(lane < sz, buf[at], edge)
            base += sx * deep

    sixth = jnp.float32(1.0 / 6.0)

    def masks(rows, lanes):
        even = (
            lax.broadcasted_iota(jnp.int32, (rows, lanes), 0)
            + lax.broadcasted_iota(jnp.int32, (rows, lanes), 1)
        ) % 2 == 0
        return even, jnp.logical_not(even)

    def beside(a, p, c, index=lambda p: p):
        rows, lanes = c.shape
        t = a[index(p - 1)] + a[index(p + 1)]
        t = t + (pltpu.roll(c, 1, 0) + pltpu.roll(c, rows - 1, 0))
        return t + (pltpu.roll(c, 1, 1) + pltpu.roll(c, lanes - 1, 1))

    def half(a, b, s, lo, hi, H, off, colour, mask, shift=None, index=lambda p: p):
        for p in range(lo, hi):
            c = a[index(p)]
            t = beside(a, p, c, index) - s[p + off]
            if shift is not None:
                t = t + shift
            b[p] = jnp.where(mask[(p - H + colour) % 2], t * sixth, c)

    fine_mask = masks(Y + 2 * R, 2 * Z)
    one_mask = masks(y1 + 2 * R, 128)

    first = [(pm, 3, 3, (X // 2, Y, Z), 5), (den, 4, 6, (X, Y, Z), 4)]
    pack(first, pk_p)
    pl.semaphore_wait(barrier, len(steps) if near else n - 1)
    exchange(first, pk_p, rk_p)()
    for k, (a, b) in enumerate(((pm, pb), (pb, pa), (pa, pb), (pb, pa))):
        d = 4 - k
        index = (lambda p: p // 2) if k == 0 else (lambda p: p)
        half(a, b, den, 6 - d, 6 + X + d, 6, 0, k % 2, fine_mask, None, index)
    pairs = []
    total = jnp.zeros((Y, Z), jnp.float32)
    for q in range(x1):
        both = None
        for p in (6 + 2 * q, 7 + 2 * q):
            c = pa[p]
            left = (den[p] - (beside(pa, p, c) - 6.0 * c))[R : R + Y, 0:Z]
            both = left if both is None else both + left
            total = total + den[p, R : R + Y, 0:Z]
        f2[2 + q, R : R + Y, 0:Z] = jnp.where(
            odd, pa[6 + 2 * q, R : R + Y, 0:Z], pa[7 + 2 * q, R : R + Y, 0:Z]
        )
        pairs.append(both)
    def halves(shape, dim, start=0):
        i = [lax.broadcasted_iota(jnp.int32, shape, k) for k in (0, 1)]
        return jnp.where((i[dim] >> 1) + start == i[1 - dim], 1.0, 0.0).astype(jnp.float32)

    to_z, to_y = halves((Z, 128), 0), halves((x1 * y1, x1 * Y), 1)
    from_z, from_y = halves((128, 2 * Z), 1), halves((Y + 2 * R, y1 + 2 * R), 0, R // 2)
    stacked = jnp.concatenate(pairs, axis=0)
    stacked = jnp.dot(stacked, to_z, precision=HI, preferred_element_type=jnp.float32)
    one = jnp.dot(to_y, stacked, precision=HI, preferred_element_type=jnp.float32) * 0.5
    for q in range(x1):
        lv[6 + q, R : R + y1, :] = one[q * y1 : (q + 1) * y1]

    second = [(lv, 5, 6, (x1, y1, z1), 5)]
    pack(second, pk_l)
    finish_second = exchange(second, pk_l, rk_l)
    fourth = [(f2, 2, 2, (X // 2, Y, Z), 4)]
    pack(fourth, pk_f)
    finish_fourth = exchange(fourth, pk_f, rk_f)
    def whole_sum(v):
        return jnp.sum(jnp.sum(v, axis=0, keepdims=True), axis=1, keepdims=True)

    gat[me, :, 128:256] = jnp.broadcast_to(whole_sum(total), (1, 128))
    finish_second()
    for p in range(6 - 4, 6 + x1 + 4):
        ea[p] = jnp.where(one_mask[p % 2], lv[p] * -sixth, 0.0)
    for k, (a, b) in enumerate(((ea, eb), (eb, ea), (ea, eb))):
        d = 3 - k
        half(a, b, lv, 6 - d, 6 + x1 + d, 6, 0, (k + 1) % 2, one_mask)
    acc = jnp.zeros((y1, 128), jnp.float32)
    for p in range(6, 6 + x1):
        c = eb[p]
        acc = acc + (lv[p] - (beside(eb, p, c) - 6.0 * c))[R : R + y1]
    for j in range(x1 // 2):
        e2[3 + j, R : R + y1, :] = jnp.where(
            odd[0:y1], eb[6 + 2 * j, R : R + y1], eb[7 + 2 * j, R : R + y1]
        )
    lane = lax.broadcasted_iota(jnp.int32, (y1, 128), 1)
    acc = jnp.where(lane < z1, acc, 0.0)

    gat[me, :, 0:128] = jnp.broadcast_to(whole_sum(acc), (1, 128))

    def spread(o, carry):
        pltpu.make_async_remote_copy(
            src_ref=gat.at[me], dst_ref=gat.at[me], send_sem=gs, recv_sem=gr,
            device_id=device(o), device_id_type=MESH,
        ).start()
        return carry

    each_other(spread)
    third = [(e2, 3, 3, (x1 // 2, y1, z1), 6)]
    pack(third, pk_e)
    finish_third = exchange(third, pk_e, rk_e)
    finish_fourth()
    finish_third()
    others = gat.at[pl.ds(0, n - 1)]
    pltpu.make_async_copy(others, others, gs).wait()
    pltpu.make_async_copy(others, others, gr).wait()

    load_op.wait()
    values = gat[:, 0, :]
    blocks = values[:, 0:128]
    mean = jnp.sum(values[:, 128:256], axis=0, keepdims=True) / jnp.float32(n * X * Y * Z)
    blocks = blocks - jnp.sum(blocks, axis=0, keepdims=True) / jnp.float32(n)
    cv[...] = jnp.dot(op_ref[...], blocks, precision=HI, preferred_element_type=jnp.float32)
    row = lax.broadcasted_iota(jnp.int32, (y1 + 2 * R, 128), 0)
    lane = lax.broadcasted_iota(jnp.int32, (y1 + 2 * R, 128), 1)
    maps = []
    for dx in (-1, 0, 1):
        by_row = []
        for dy in (-1, 0, 1):
            vals = []
            for dz in (-1, 0, 1):
                at = (xs[dx] * ny + ys[dy]) * nz
                vals.append(cv[pl.ds(at + zs[dz], 1), :])
            by_row.append(jnp.where(lane < z1, vals[1], jnp.where(lane < (z1 + 128) // 2, vals[2], vals[0])))
        maps.append(jnp.where(row < R, by_row[0], jnp.where(row < R + y1, by_row[1], by_row[2])))
    for p in range(0, x1 + 12):
        which = 0 if p < 6 else (1 if p < 6 + x1 else 2)
        ea[p] = e2[p // 2] + (maps[which] + mean * jnp.float32(8.0 / 3.0))
    for k, (a, b) in enumerate(((ea, eb), (eb, ea), (ea, eb), (eb, ea))):
        d = 5 - k
        half(a, b, lv, 6 - d, 6 + x1 + d, 6, 0, k % 2, one_mask, 4.0 * mean)

    mean2 = jnp.concatenate([mean, mean], axis=1)
    for q in range(4, 6 + x1 + 2):
        wide = jnp.dot(ea[q], from_z, precision=HI, preferred_element_type=jnp.float32)
        wide = jnp.dot(from_y, wide, precision=HI, preferred_element_type=jnp.float32)
        wide = wide + mean2 * jnp.float32(2.0 / 3.0)
        for p in (2 * (q - 4), 2 * (q - 4) + 1):
            pb[p] = f2[p // 2] + wide
    for k, (a, b) in enumerate(((pb, pa), (pa, pb), (pb, pa))):
        d = 3 - k
        half(a, b, den, 4 - d, 4 + X + d, 4, 2, k % 2, fine_mask, mean2)
    for p in range(4, 4 + X):
        c = pa[p]
        t = (beside(pa, p, c) - den[p + 2] + mean2) * sixth
        out_ref[p - 4] = jnp.where(fine_mask[(p - 3) % 2], t, c)[R : R + Y, 0:Z]


def body(dims, density, potential):
    nx, ny, nz, X, Y, Z = dims
    n = nx * ny * nz
    x1, y1, z1 = X // 2, Y // 2, Z // 2
    op = coarse_operator(nx, ny, nz, float(y1 * z1), float(x1 * z1), float(x1 * y1))
    rows, rows1 = Y + 2 * R, y1 + 2 * R
    f32 = jnp.float32
    fine, one = (Y, 128), (y1, 128)
    vmem = pl.BlockSpec(memory_space=pltpu.VMEM)
    return pl.pallas_call(
        functools.partial(kernel, dims),
        out_shape=pltpu.VMEM((X, Y, Z), f32),
        in_specs=[pl.BlockSpec(memory_space=pl.ANY)] * 3,
        out_specs=vmem,
        scratch_shapes=[
            pltpu.VMEM((n, n), f32),
            pltpu.VMEM((X, Y, Z), f32),
            pltpu.VMEM((X // 2 + 6, rows, 2 * Z), f32),
            pltpu.VMEM((X + 12, rows, 2 * Z), f32),
            pltpu.VMEM((X + 12, rows, 2 * Z), f32),
            pltpu.VMEM((X + 12, rows, 2 * Z), f32),
            pltpu.VMEM((x1 + 12, rows1, 128), f32),
            pltpu.VMEM((x1 + 12, rows1, 128), f32),
            pltpu.VMEM((x1 + 12, rows1, 128), f32),
            pltpu.VMEM((x1 // 2 + 6, rows1, 128), f32),
            pltpu.VMEM((X // 2 + 4, rows, 2 * Z), f32),
            pltpu.VMEM((n, 1, 256), f32),
            pltpu.VMEM((n, 128), f32),
        ]
        + [pltpu.VMEM(lead + s, f32) for lead in ((2,), (2, 3, 3)) for s in (fine, one, one, fine)]
        + [
            pltpu.SemaphoreType.DMA((82,)),
            pltpu.SemaphoreType.DMA((82,)),
            pltpu.SemaphoreType.DMA,
            pltpu.SemaphoreType.DMA,
            pltpu.SemaphoreType.DMA((3,)),
        ],
        compiler_params=pltpu.CompilerParams(collective_id=0, has_side_effects=True),
        name="vcycle",
    )(density, potential, op)


def solution(mesh):
    nx, ny, nz = (mesh.shape[a] for a in ("gx", "gy", "gz"))

    def run(density, potential):
        return body((nx, ny, nz) + density.shape, density, potential)

    spec = P("gx", "gy", "gz")
    return jax.shard_map(run, mesh=mesh, in_specs=(spec, spec), out_specs=spec, check_vma=False)
```

```python
import functools
import numpy as np
import jax
import jax.numpy as jnp
from jax import lax
from jax.experimental import pallas as pl
from jax.experimental.pallas import tpu as pltpu
from jax.sharding import PartitionSpec as P

HI = lax.Precision.HIGHEST
MESH = pl.DeviceIdType.MESH
H, H1 = 4, 8
SIDES = ((0, 1), (0, -1), (1, 0), (-1, 0), (1, 1), (1, -1), (-1, 1), (-1, -1), (0, 0))


def table(count):
    modes = (np.arange(count) + 1) // 2
    angle = 2 * np.pi * np.outer(np.arange(count), modes) / count
    q = np.where(np.arange(count) % 2 == 1, np.cos(angle), np.sin(angle)) * np.sqrt(2 / count)
    q = np.where(2 * modes == count, np.cos(angle) / np.sqrt(count), q)
    q[:, 0] = 1 / np.sqrt(count)
    return q, 2 - 2 * np.cos(2 * np.pi * modes / count)


def coarse_operator(nx, ny, nz, wx, wy, wz):
    qx, lx = table(nx)
    qy, ly = table(ny)
    qz, lz = table(nz)
    q = np.kron(np.kron(qx, qy), qz)
    lam = wx * lx[:, None, None] + wy * ly[None, :, None] + wz * lz[None, None, :]
    lam = lam.reshape(-1)
    inv = np.concatenate([[0.0], -1.0 / lam[1:]])
    return ((q * inv) @ q.T).astype(np.float32)


def turn(v, shift):
    shift %= 128
    return pltpu.roll(v, shift, 1) if shift else v


def kernel(
    dims, den_hbm, pot_hbm, op_hbm, out_ref,
    den_v, pot_v, op_v, cp, cd, cf, cl, ce,
    z1s, z1r, zfs, zfr, zls, zlr, zes, zer,
    R, B, SR, SB, lv, ea, e2, gat, cv, dummy,
    ssem, rsem, lsem,
):
    nx, ny, nz, X, Y, Z = dims
    n = nx * ny * nz
    I, J, K = X // 2, Y // 2, Z // 2
    T, T1 = J + 2 * H, J + 2 * H1
    M = I // 2
    U = (M + 1) // 2
    G, F = X // 4, max(X // 12, 1)
    FW = X // F
    assert X % 4 == 0 and FW <= 12 and I <= 12 and 2 * K <= 128 and J % 8 == 0
    ix, iy, iz = lax.axis_index("gx"), lax.axis_index("gy"), lax.axis_index("gz")
    me = (ix * ny + iy) * nz + iz

    def around(i, count):
        return [i] + [jnp.where(i + o >= count, i + o - count, i + o) for o in range(1, count)]

    xs, ys, zs = around(ix, nx), around(iy, ny), around(iz, nz)

    def device(o):
        if isinstance(o, int):
            return (xs[o // (ny * nz)], ys[o // nz % ny], zs[o % nz])
        ox, oy, oz = o // (ny * nz), (o // nz) % ny, o % nz
        return (lax.rem(ix + ox, nx), lax.rem(iy + oy, ny), lax.rem(iz + oz, nz))

    def each_other(step):
        if n <= 64:
            for o in range(1, n):
                step(o, 0)
        else:
            lax.fori_loop(1, n, step, 0)

    wide = (lambda ref: ref) if Z == 128 else (lambda ref: ref.at[:, :, pl.ds(0, Z)])
    load_p = pltpu.make_async_copy(pot_hbm, wide(pot_v), lsem.at[0])
    load_d = pltpu.make_async_copy(den_hbm, wide(den_v), lsem.at[1])
    load_op = pltpu.make_async_copy(op_hbm, op_v, lsem.at[2])
    load_p.start()
    load_d.start()
    load_op.start()

    barrier = pltpu.get_barrier_semaphore()

    def greet(o, carry):
        pl.semaphore_signal(barrier, inc=1, device_id=device(o), device_id_type=MESH)
        return carry

    near = max(nx, ny, nz) <= 5
    steps = sorted({
        (dx % nx * ny + dy % ny) * nz + dz % nz
        for dx in (-1, 0, 1) for dy in (-1, 0, 1) for dz in (-1, 0, 1)
    } - {0})
    if near:
        for o in steps:
            greet(o, 0)
    else:
        each_other(greet)

    class Exchange:
        def __init__(self, k):
            self.k, self.rows = k, 0

        def send(self, src, dst, at, to):
            dx, dy, dz = to
            copy = pltpu.make_async_remote_copy(
                src_ref=src, dst_ref=dst, send_sem=ssem.at[self.k], recv_sem=rsem.at[self.k],
                device_id=(xs[dx], ys[dy], zs[dz]), device_id_type=MESH,
            )
            copy.start()
            self.rows += at

        def wait(self):
            all_of = dummy.at[pl.ds(0, self.rows)]
            pltpu.make_async_copy(all_of, all_of, rsem.at[self.k]).wait()
            pltpu.make_async_copy(all_of, all_of, ssem.at[self.k]).wait()

    def part(d, own, count, first):
        if d == 0:
            return first, own, first
        if d == 1:
            return first + own - count, count, first - count
        return first, count, first + own

    def block(ex, src, dst, px, py, to, shift=0, lead=None):
        (sx, cx, tx), (sy, cy, ty) = px, py
        target = dst if lead is None else dst.at[lead]
        ex.send(
            src.at[pl.ds(sx, cx), pl.ds(sy - shift, cy)],
            target.at[pl.ds(tx, cx), pl.ds(ty, cy)],
            cx * cy, to,
        )

    def iota(rows, dim):
        return lax.broadcasted_iota(jnp.int32, (rows, 128), dim)

    lane = {rows: iota(rows, 1) for rows in {J, T, T1}}

    def place(acc, v, pieces):
        by_shift = {}
        for src, dst, width in pieces:
            by_shift.setdefault((dst - src) % 128, []).append((dst, width))
        at = lane[v.shape[0]]
        for shift, spans in by_shift.items():
            mask = None
            for dst, width in spans:
                inside = (at >= dst) & (at < dst + width)
                mask = inside if mask is None else mask | inside
            moved = turn(v, shift)
            acc = jnp.where(mask, moved, acc)
        return acc

    def outside(z, right, left):
        if (right - left) % 128 == 0:
            return turn(z, right)
        return jnp.where(lane[z.shape[0]] < 96, turn(z, right), turn(z, left))

    def with_sides(v, half, z, right, left):
        own = turn(v, -K) if half else v
        if z is None:
            return own
        return jnp.where(lane[v.shape[0]] < K, own, outside(z, right, left))

    def two(a, b):
        return jnp.where(lane[a.shape[0]] < K, a, turn(b, K))

    l8 = lane[J]
    low = jnp.where(l8 < K, 2 * l8, 2 * (l8 - K) + 1) & 127
    high = jnp.where(l8 < K, 2 * l8 + 1, 2 * (l8 - K)) & 127
    order = (low, high)

    def colours(ref, x, which):
        v = [ref[x, pl.ds(b, J, stride=2), :] for b in (0, 1)]
        take = [jnp.take_along_axis(u, order[which], axis=1, mode="promise_in_bounds") for u in v]
        return jnp.where(l8 < K, take[0], take[1])

    def tile(x, t):
        forward = 0 <= x < X // 2 or x >= X
        return 2 * (x + 4) + (t if forward else 1 - t)

    load_p.wait()
    load_d.wait()
    total = jnp.zeros((J, 128), jnp.float32)
    for g in range(G):
        acc = jnp.zeros((J, 128), jnp.float32)
        for q in range(4):
            x = 4 * g + q
            black = colours(pot_v, x, 1 - x % 2)
            dens = [colours(den_v, x, x % 2), colours(den_v, x, 1 - x % 2)]
            cp[x + 5, H : H + J] = black
            acc = place(acc, black, [
                p for h in (0, 1)
                for p in ((h * K, 15 * q + 3 * h, 3), (h * K + K - 3, 61 + 15 * q + 3 * h, 3))
            ])
            for t in (0, 1):
                cd[tile(x, t), H : H + J] = dens[t]
                total = total + dens[t]
                acc = place(acc, dens[t], [
                    p for h in (0, 1) for o in (15 * q + 6 + 4 * t + 2 * h,)
                    for p in ((h * K, o, 2), (h * K + K - 2, 62 + o, 2))
                ])
        z1s[g] = acc
    total = jnp.where(l8 < 2 * K, total, 0.0)

    pl.semaphore_wait(barrier, len(steps) if near else n - 1)
    first = Exchange(0)
    for dx, dy in SIDES:
        if dx or dy:
            edge = dx != 0 and dy != 0
            block(first, cp, cp, part(dx, X, 4 if edge else 5, 5), part(dy, J, 2 if edge else 3, H), (dx, dy, 0))
            block(first, cd, cd, part(dx, 2 * X, 5 if edge else 7, 8), part(dy, J, 2, H), (dx, dy, 0))
        for dz in (1, -1):
            g0, gn, g1 = part(dx, G, 1, 1)
            block(first, z1s, z1r, (g0 - 1, gn, g1), part(dy, J, 2, H), (dx, dy, dz), H, max(dz, 0))
    first.wait()

    def base(x, b):
        return 8 + ((x + 5) * 2 + b) * T

    def get(ref, x, b, off=0):
        return ref[pl.ds(base(x, b) + off, T), :]

    def own(ref, x, b, off=0):
        return ref[pl.ds(base(x, b) + H + off, J), :]

    sides = {}

    def side(x):
        g = x // 4 + 1
        if g not in sides:
            sides[g] = jnp.where(lane[T] < 60, z1r[0, g], z1r[1, g])
        return sides[g]

    for x in range(-5, X + 5):
        far = max(-x, x - X + 1, 0)
        z = side(x) if far < 5 else None
        for h in (0, 1):
            s = 15 * (x % 4) + 3 * h
            B[pl.ds(base(x, h), T), :] = with_sides(cp[x + 5], h, z, K - s, 64 - s)
        for t, ref in ((0, SR), (1, SB)):
            if far <= 4 - t:
                for h in (0, 1):
                    s = 15 * (x % 4) + 6 + 4 * t + 2 * h
                    ref[pl.ds(base(x, h), T), :] = with_sides(cd[tile(x, t)], h, z, K - s, 64 - s)

    sixth = jnp.float32(1.0 / 6.0)

    def beside(read, v, x, b, colour):
        c = (x + b + colour) % 2
        mid = read(v, x, b)
        t = read(v, x - 1, b) + read(v, x + 1, b)
        t = t + (read(v, x, 1 - b) + read(v, x, 1 - b, 2 * b - 1))
        return t + (mid + turn(mid, 1 - 2 * c))

    def half(depth, colour):
        new, old, src = ((R, B, SR), (B, R, SB))[colour]
        for x in range(-depth, X + depth):
            for b in (0, 1):
                new[pl.ds(base(x, b), T), :] = (beside(get, old, x, b, colour) - get(src, x, b)) * sixth

    for k in range(4):
        half(4 - k, k % 2)

    def base1(p):
        return 8 + (p + 6) * T1

    def get1(ref, p, off=0):
        return ref[pl.ds(base1(p) + off, T1), :]

    one = []
    for i in range(I):
        left = None
        for x in (2 * i, 2 * i + 1):
            for b in (0, 1):
                for colour, (v, w, s) in enumerate(((R, B, SR), (B, R, SB))):
                    r = own(s, x, b) - (beside(own, w, x, b, colour) - 6.0 * own(v, x, b))
                    left = r if left is None else left + r
        one.append(left * 0.5)
    hi = 59 if 5 * I <= 59 else 64
    acc = jnp.zeros((J, 128), jnp.float32)
    for i in range(I):
        acc = place(acc, one[i], [(0, 5 * i, 5), (K - 5, hi + 5 * i, 5)])
    zls[0] = acc
    for m in range(M):
        cl[3 + m, H1 : H1 + J] = two(one[2 * m], one[2 * m + 1])

    once = nx == 2 and M == 3
    xsides = [(dx, dy) for dx, dy in SIDES if dx >= 0 or nx > 2]

    def slots(dx, single):
        if not single:
            return part(dx, 1, 1, 1)
        return (1, 1, 1) if dx == 0 else (1, 1, 0)

    second = Exchange(1)
    for dx, dy in (xsides if once else SIDES):
        px = (3, M, 0) if once and dx else part(dx, M, 3, 3)
        if dx or dy:
            block(second, cl, cl, px, part(dy, J, 4 if dx else 5, H1), (dx, dy, 0))
        if dx >= 0 or nx > 2:
            for dz in (1, -1):
                s0, sn, s1 = slots(dx, nx == 2)
                block(second, zls, zlr, (s0 - 1, sn, s1), part(dy, J, 3 if dx else 4, H1), (dx, dy, dz), H1, max(dz, 0))

    for f in range(F):
        acc = jnp.zeros((J, 128), jnp.float32)
        for q in range(FW):
            x = f * FW + q
            v = two(own(B, x, 0), own(B, x, 1))
            cf[x + 4, H : H + J] = v
            acc = place(acc, v, [
                p for h in (0, 1) for o in (4 * q + 2 * h,)
                for p in ((h * K, o, 2), (h * K + K - 2, 62 + o, 2))
            ])
        zfs[f] = acc

    second.wait()
    fourth = Exchange(3)
    for dx, dy in SIDES:
        if dx or dy:
            edge = dx != 0 and dy != 0
            block(fourth, cf, cf, part(dx, X, 3 if edge else 4, 4), part(dy, J, 2, H), (dx, dy, 0))
        for dz in (1, -1):
            g0, gn, g1 = part(dx, F, 1, 1)
            block(fourth, zfs, zfr, (g0 - 1, gn, g1), part(dy, J, 2, H), (dx, dy, dz), H, max(dz, 0))

    def slot_of(p, count):
        if p < 0:
            return 0, p + count
        if p >= count:
            return (0 if nx == 2 else 2), p - count
        return 1, p

    zl = [jnp.where(lane[T1] < hi, zlr[0, s], zlr[1, s]) for s in range(2 if nx == 2 else 3)]
    for p in range(-5, I + 5):
        slot, i = slot_of(p, I)
        m = i // 2
        at = 3 + m if slot == 1 else (m - (M - 3) if p < 0 or once else 3 + M + m)
        lv[pl.ds(base1(p), T1), :] = with_sides(cl[at], i % 2, zl[slot], K - 5 * i, 123 - hi - 5 * i)

    even = (iota(T1, 0) + lane[T1]) % 2 == 0
    mask = (even, jnp.logical_not(even))

    def beside1(read, v, p, c):
        t = read(v, p - 1) + read(v, p + 1)
        t = t + (read(v, p, -1) + read(v, p, 1))
        return t + (turn(c, 1) + turn(c, -1))

    def half1(depth, colour, shift=None, read=get1, src=ea):
        for p in range(-depth, I + depth):
            c = read(src, p)
            t = beside1(read, src, p, c) - get1(lv, p)
            if shift is not None:
                t = t + shift
            ea[pl.ds(base1(p), T1), :] = jnp.where(mask[(p + colour) % 2], t * sixth, c)

    for p in range(-4, I + 4):
        ea[pl.ds(base1(p), T1), :] = jnp.where(mask[p % 2], get1(lv, p) * -sixth, 0.0)
    for depth, colour in ((3, 1), (2, 0), (1, 1)):
        half1(depth, colour)

    def own1(ref, p, off=0):
        return ref[pl.ds(base1(p) + H1 + off, J), :]

    acc = jnp.zeros((J, 128), jnp.float32)
    for p in range(I):
        c = own1(ea, p)
        acc = acc + (own1(lv, p) - (beside1(own1, ea, p, c) - 6.0 * c))
    acc = jnp.where(l8 < K, acc, 0.0)

    def whole_sum(v):
        return jnp.sum(jnp.sum(v, axis=0, keepdims=True), axis=1, keepdims=True)

    lane1 = lax.broadcasted_iota(jnp.int32, (1, 128), 1)
    gat[me] = jnp.where(lane1 < 64, whole_sum(acc), whole_sum(total))

    def spread(o, carry):
        pltpu.make_async_remote_copy(
            src_ref=gat.at[me], dst_ref=gat.at[me], send_sem=ssem.at[4], recv_sem=rsem.at[4],
            device_id=device(o), device_id_type=MESH,
        ).start()
        return carry

    each_other(spread)

    odd = (iota(J, 0) + l8) % 2 == 1
    black = [jnp.where(odd, own1(ea, 2 * m), own1(ea, 2 * m + 1)) for m in range(M)]
    acc = jnp.zeros((J, 128), jnp.float32)
    for m in range(M):
        acc = place(acc, black[m], [(0, 6 * m, 6), (K - 6, 58 + 6 * m, 6)])
    zes[0] = acc
    for u in range(U):
        ce[2 + u, H1 : H1 + J] = two(black[2 * u], black[2 * u + 1]) if 2 * u + 1 < M else black[2 * u]
    third = Exchange(2)
    once3 = nx == 2 and U == 2
    for dx, dy in (xsides if once3 else SIDES):
        px = (2, U, 0) if once3 and dx else part(dx, U, 2, 2)
        if dx or dy:
            block(third, ce, ce, px, part(dy, J, 5 if dx else 6, H1), (dx, dy, 0))
        if dx >= 0 or nx > 2:
            for dz in (1, -1):
                s0, sn, s1 = slots(dx, nx == 2)
                block(third, zes, zer, (s0 - 1, sn, s1), part(dy, J, 4 if dx else 5, H1), (dx, dy, dz), H1, max(dz, 0))

    fourth.wait()
    for x in range(-4, X + 4):
        far = max(-x, x - X + 1, 0)
        z = None
        if far < 4:
            f = 0 if x < 0 else (F + 1 if x >= X else x // FW + 1)
            if ("f", f) not in sides:
                sides["f", f] = jnp.where(lane[T] < 60, zfr[0, f], zfr[1, f])
            z = sides["f", f]
        for h in (0, 1):
            s = 4 * (x % FW) + 2 * h
            B[pl.ds(base(x, h), T), :] = with_sides(cf[x + 4], h, z, K - s, 64 - s)

    third.wait()
    others = gat.at[pl.ds(0, n - 1)]
    pltpu.make_async_copy(others, others, ssem.at[4]).wait()
    pltpu.make_async_copy(others, others, rsem.at[4]).wait()
    load_op.wait()
    values = gat[:, 0, :]
    swapped = pltpu.roll(values, 64, 1)
    below = lax.broadcasted_iota(jnp.int32, (n, 128), 1) < 64
    blocks = jnp.where(below, values, swapped)
    mean = jnp.sum(jnp.where(below, swapped, values), axis=0, keepdims=True) / jnp.float32(n * X * Y * Z)
    blocks = blocks - jnp.sum(blocks, axis=0, keepdims=True) / jnp.float32(n)
    cv[...] = jnp.dot(op_v[...], blocks, precision=HI, preferred_element_type=jnp.float32)
    row = iota(T1, 0)
    at = lane[T1]
    maps = []
    for dx in (-1, 0, 1):
        by_row = []
        for dy in (-1, 0, 1):
            vals = []
            for dz in (-1, 0, 1):
                o = (xs[dx] * ny + ys[dy]) * nz
                vals.append(cv[pl.ds(o + zs[dz], 1), :])
            by_row.append(jnp.where(at < K, vals[1], jnp.where(at < (K + 128) // 2, vals[2], vals[0])))
        field = jnp.where(row < H1, by_row[0], jnp.where(row < H1 + J, by_row[1], by_row[2]))
        maps.append(field + mean * jnp.float32(8.0 / 3.0))

    def base2(m):
        return 8 + (m + 3) * T1

    ze = [jnp.where(lane[T1] < 58, zer[0, s], zer[1, s]) for s in range(2 if nx == 2 else 3)]
    for mm in range(-3, M + 3):
        slot, m = slot_of(mm, M)
        u = m // 2
        at = 2 + u if slot == 1 else (u - (U - 2) if mm < 0 or once3 else 2 + U + u)
        v = with_sides(ce[at], m % 2, ze[slot], K - 6 * m, 64 - 6 * m)
        e2[pl.ds(base2(mm), T1), :] = v + maps[0 if mm < 0 else (1 if mm < M else 2)]

    def get2(ref, p, off=0):
        return ref[pl.ds(base2(p // 2) + off, T1), :]

    shift = 4.0 * mean
    half1(5, 0, shift, get2, e2)
    for depth, colour in ((4, 1), (3, 0), (2, 1)):
        half1(depth, colour, shift)

    rise = mean * jnp.float32(2.0 / 3.0)
    for i in range(-2, I + 2):
        e = ea[pl.ds(base1(i) + H1 - H, T), :] + rise
        for x in (2 * i, 2 * i + 1):
            for b in (0, 1):
                B[pl.ds(base(x, b), T), :] = get(B, x, b) + e

    def last(depth, colour):
        new, old, src = ((R, B, SR), (B, R, SB))[colour]
        for x in range(-depth, X + depth):
            for b in (0, 1):
                t = beside(get, old, x, b, colour) - get(src, x, b) + mean
                new[pl.ds(base(x, b), T), :] = t * sixth

    last(3, 0)
    last(2, 1)
    last(1, 0)
    back = l8 >> 1
    odd_lane = (l8 & 1) == 1
    for x in range(X):
        for b in (0, 1):
            red = own(R, x, b)
            dark = (beside(own, R, x, b, 1) - own(SB, x, b) + mean) * sixth
            pair = (red, dark) if (x + b) % 2 == 0 else (dark, red)
            e, o = (jnp.take_along_axis(v, back, axis=1, mode="promise_in_bounds") for v in pair)
            out_ref[x, pl.ds(b, J, stride=2), :] = jnp.where(odd_lane, o, e)[:, 0:Z]


def body(dims, density, potential):
    nx, ny, nz, X, Y, Z = dims
    n = nx * ny * nz
    I, J, K = X // 2, Y // 2, Z // 2
    T, T1 = J + 2 * H, J + 2 * H1
    M = I // 2
    U = (M + 1) // 2
    G, F = X // 4, max(X // 12, 1)
    op = coarse_operator(nx, ny, nz, float(J * K), float(I * K), float(I * J))
    fine = 16 + (X + 10) * 2 * T
    coarse = 16 + (I + 12) * T1

    def vmem(*shape):
        return pltpu.VMEM(shape, jnp.float32)

    return pl.pallas_call(
        functools.partial(kernel, dims),
        out_shape=pltpu.VMEM((X, Y, Z), jnp.float32),
        in_specs=[pl.BlockSpec(memory_space=pl.ANY)] * 3,
        out_specs=pl.BlockSpec(memory_space=pltpu.VMEM),
        scratch_shapes=[
            vmem(X, Y, 128),
            vmem(X, Y, 128),
            vmem(n, n),
            vmem(X + 10, T, 128),
            vmem(2 * (X + 8), T, 128),
            vmem(X + 8, T, 128),
            vmem(M + 6, T1, 128),
            vmem(U + 4, T1, 128),
            vmem(G, J, 128),
            vmem(2, G + 2, T, 128),
            vmem(F, J, 128),
            vmem(2, F + 2, T, 128),
            vmem(1, J, 128),
            vmem(2, 3, T1, 128),
            vmem(1, J, 128),
            vmem(2, 3, T1, 128),
            vmem(fine, 128),
            vmem(fine, 128),
            vmem(fine, 128),
            vmem(fine, 128),
            vmem(coarse, 128),
            vmem(coarse, 128),
            vmem(16 + (M + 6) * T1, 128),
            vmem(n, 1, 128),
            vmem(n, 128),
            vmem(2048, 128),
            pltpu.SemaphoreType.DMA((5,)),
            pltpu.SemaphoreType.DMA((5,)),
            pltpu.SemaphoreType.DMA((3,)),
        ],
        compiler_params=pltpu.CompilerParams(collective_id=0, has_side_effects=True),
        name="vcycle",
    )(density, potential, op)


def solution(mesh):
    nx, ny, nz = (mesh.shape[a] for a in ("gx", "gy", "gz"))

    def run(density, potential):
        return body((nx, ny, nz) + density.shape, density, potential)

    spec = P("gx", "gy", "gz")
    return jax.shard_map(run, mesh=mesh, in_specs=(spec, spec), out_specs=spec, check_vma=False)
```

```python
import functools
import numpy as np
import jax
import jax.numpy as jnp
from jax import lax
from jax.experimental import pallas as pl
from jax.experimental.pallas import tpu as pltpu
from jax.sharding import PartitionSpec as P

HI = lax.Precision.HIGHEST
MESH = pl.DeviceIdType.MESH
H, H1 = 4, 12
DEEP = 9
SIDES = ((1, 1), (1, -1), (-1, 1), (-1, -1), (0, 1), (0, -1), (0, 0), (1, 0), (-1, 0))


def table(count):
    modes = (np.arange(count) + 1) // 2
    angle = 2 * np.pi * np.outer(np.arange(count), modes) / count
    q = np.where(np.arange(count) % 2 == 1, np.cos(angle), np.sin(angle)) * np.sqrt(2 / count)
    q = np.where(2 * modes == count, np.cos(angle) / np.sqrt(count), q)
    q[:, 0] = 1 / np.sqrt(count)
    return q, 2 - 2 * np.cos(2 * np.pi * modes / count)


def coarse_operator(nx, ny, nz, wx, wy, wz):
    qx, lx = table(nx)
    qy, ly = table(ny)
    qz, lz = table(nz)
    q = np.kron(np.kron(qx, qy), qz)
    lam = wx * lx[:, None, None] + wy * ly[None, :, None] + wz * lz[None, None, :]
    lam = lam.reshape(-1)
    inv = np.concatenate([[0.0], -1.0 / lam[1:]])
    return ((q * inv) @ q.T).astype(np.float32)


def offsets(nx, ny, nz):
    steps = [(dx % nx, dy % ny, dz % nz) for dx in (0, 1, -1) for dy in (0, 1, -1) for dz in (0, 1, -1)]
    return list(dict.fromkeys(steps))


def residual_weights(nx, ny, nz, I, J, K):
    block = np.zeros((3 * I, 3 * J, 3 * K))
    block[I : 2 * I, J : 2 * J, K : 2 * K] = 1.0

    def beside(v):
        return sum(np.roll(v, d, axis) for axis in range(3) for d in (1, -1))

    red = np.indices(block.shape).sum(0) % 2 == 0
    v = beside(block) - 6.0 * block
    black2 = np.where(red, 0.0, v)
    red2 = np.where(red, v + beside(black2) / 6.0, 0.0)
    black1 = np.where(red, 0.0, beside(red2) / 6.0)
    red1 = np.where(red, beside(black1) / 6.0, 0.0)
    w = block + (black2 + red2 + black1 + red1) / 6.0
    names = offsets(nx, ny, nz)
    own = np.zeros((len(names), I, J, K))
    for dx in (0, 1, -1):
        for dy in (0, 1, -1):
            for dz in (0, 1, -1):
                x, y, z = (1 - dx) * I, (1 - dy) * J, (1 - dz) * K
                own[names.index((dx % nx, dy % ny, dz % nz))] += w[x : x + I, y : y + J, z : z + K]
    even = np.indices((J, K)).sum(0) % 2 == 0
    first, second = own[:, 0::2], own[:, 1::2]
    out = np.zeros((len(names), I // 2, J, 128))
    out[..., :K] = np.where(even, first, second)
    out[..., K : 2 * K] = np.where(even, second, first)
    return out.astype(np.float32)


def coarse_weights(op, nx, ny, nz):
    names = offsets(nx, ny, nz)
    green = op.astype(np.float64)[:, 0].reshape(nx, ny, nz)
    rx, ry, rz = np.indices((nx, ny, nz)).reshape(3, -1)
    out = np.zeros((len(names), nx * ny * nz, 128))
    for o, (ox, oy, oz) in enumerate(names):
        for f, (fx, fy, fz) in enumerate(names):
            out[o, :, f] = green[(ox - rx - fx) % nx, (oy - ry - fy) % ny, (oz - rz - fz) % nz]
    return out.astype(np.float32)


def turn(v, shift):
    shift %= 128
    return pltpu.roll(v, shift, 1) if shift else v


def kernel(
    dims, den_hbm, pot_hbm, rw_hbm, cw_hbm, out_ref,
    den_v, pot_v, rw, cw, cp, cd, cf, cl,
    z1s, z1r, zfs, zfr, zls, zlr,
    R, B, SR, SB, LR, LB, ER, EB, gat, cv, dummy,
    ssem, rsem, lsem,
):
    nx, ny, nz, X, Y, Z = dims
    n = nx * ny * nz
    I, J, K = X // 2, Y // 2, Z // 2
    T, T1 = J + 2 * H, J + 2 * H1
    M = I // 2
    ring = nx == 2 and I < DEEP
    E = 0 if ring else 5
    G, F, GL = X // 4, max(X // 12, 1), M // 3
    FW = X // F
    assert X % 12 == 0 and FW <= 12 and 2 * K <= 128 and J % 8 == 0 and 2 * J > DEEP and 2 * M >= E and M % 3 == 0
    names = offsets(nx, ny, nz)
    NF = len(names)
    Q = -(-(NF + 1) // 8) * 8
    ix, iy, iz = lax.axis_index("gx"), lax.axis_index("gy"), lax.axis_index("gz")
    me = (ix * ny + iy) * nz + iz

    def around(i, count):
        return [i] + [jnp.where(i + o >= count, i + o - count, i + o) for o in range(1, count)]

    xs, ys, zs = around(ix, nx), around(iy, ny), around(iz, nz)

    def device(o):
        if isinstance(o, int):
            return (xs[o // (ny * nz)], ys[o // nz % ny], zs[o % nz])
        ox, oy, oz = o // (ny * nz), (o // nz) % ny, o % nz
        return (lax.rem(ix + ox, nx), lax.rem(iy + oy, ny), lax.rem(iz + oz, nz))

    def each_other(step):
        if n <= 64:
            for o in range(1, n):
                step(o, 0)
        else:
            lax.fori_loop(1, n, step, 0)

    wide = (lambda ref: ref) if Z == 128 else (lambda ref: ref.at[:, :, pl.ds(0, Z)])
    load_p = pltpu.make_async_copy(pot_hbm, wide(pot_v), lsem.at[0])
    load_d = pltpu.make_async_copy(den_hbm, wide(den_v), lsem.at[1])
    load_rw = pltpu.make_async_copy(rw_hbm, rw, lsem.at[2])
    load_cw = pltpu.make_async_copy(cw_hbm, cw, lsem.at[3])
    load_p.start()
    load_d.start()
    load_rw.start()
    load_cw.start()

    barrier = pltpu.get_barrier_semaphore()

    def greet(o, carry):
        pl.semaphore_signal(barrier, inc=1, device_id=device(o), device_id_type=MESH)
        return carry

    near = max(nx, ny, nz) <= 5
    steps = sorted({
        (dx % nx * ny + dy % ny) * nz + dz % nz
        for dx in (-1, 0, 1) for dy in (-1, 0, 1) for dz in (-1, 0, 1)
    } - {0})
    if near:
        for o in steps:
            greet(o, 0)
    else:
        each_other(greet)

    class Exchange:
        def __init__(self, k):
            self.k, self.rows = k, 0

        def send(self, src, dst, at, to):
            dx, dy, dz = to
            copy = pltpu.make_async_remote_copy(
                src_ref=src, dst_ref=dst, send_sem=ssem.at[self.k], recv_sem=rsem.at[self.k],
                device_id=(xs[dx], ys[dy], zs[dz]), device_id_type=MESH,
            )
            copy.start()
            self.rows += at

        def wait(self):
            all_of = dummy.at[pl.ds(0, self.rows)]
            pltpu.make_async_copy(all_of, all_of, rsem.at[self.k]).wait()
            pltpu.make_async_copy(all_of, all_of, ssem.at[self.k]).wait()

    def part(d, own, count, first):
        if d == 0:
            return first, own, first
        if d == 1:
            return first + own - count, count, first - count
        return first, count, first + own

    def block(ex, src, dst, px, py, to, shift=0, lead=None):
        (sx, cx, tx), (sy, cy, ty) = px, py
        target = dst if lead is None else dst.at[lead]
        ex.send(
            src.at[pl.ds(sx, cx), pl.ds(sy - shift, cy)],
            target.at[pl.ds(tx, cx), pl.ds(ty, cy)],
            cx * cy, to,
        )

    def iota(rows, dim):
        return lax.broadcasted_iota(jnp.int32, (rows, 128), dim)

    lane = {rows: iota(rows, 1) for rows in {J, T, T1}}

    def place(acc, v, pieces):
        by_shift = {}
        for src, dst, width in pieces:
            by_shift.setdefault((dst - src) % 128, []).append((dst, width))
        at = lane[v.shape[0]]
        for shift, spans in by_shift.items():
            mask = None
            for dst, width in spans:
                inside = (at >= dst) & (at < dst + width)
                mask = inside if mask is None else mask | inside
            moved = turn(v, shift)
            acc = jnp.where(mask, moved, acc)
        return acc

    def outside(z, right, left):
        if (right - left) % 128 == 0:
            return turn(z, right)
        return jnp.where(lane[z.shape[0]] < 96, turn(z, right), turn(z, left))

    def with_sides(v, half, z, right, left):
        own = turn(v, -K) if half else v
        if z is None:
            return own
        return jnp.where(lane[v.shape[0]] < K, own, outside(z, right, left))

    def two(a, b):
        return jnp.where(lane[a.shape[0]] < K, a, turn(b, K))

    l8 = lane[J]
    low = jnp.where(l8 < K, 2 * l8, 2 * (l8 - K) + 1) & 127
    high = jnp.where(l8 < K, 2 * l8 + 1, 2 * (l8 - K)) & 127
    order = (low, high)

    def colours(ref, x, which):
        v = [ref[x, pl.ds(b, J, stride=2), :] for b in (0, 1)]
        take = [jnp.take_along_axis(u, order[which], axis=1, mode="promise_in_bounds") for u in v]
        return jnp.where(l8 < K, take[0], take[1])

    def tile(x, t):
        forward = 0 <= x < X // 2 or x >= X
        return 2 * (x + 4) + (t if forward else 1 - t)

    load_p.wait()
    load_d.wait()
    total = jnp.zeros((J, 128), jnp.float32)
    for g in range(G):
        acc = jnp.zeros((J, 128), jnp.float32)
        for q in range(4):
            x = 4 * g + q
            black = colours(pot_v, x, 1 - x % 2)
            dens = [colours(den_v, x, x % 2), colours(den_v, x, 1 - x % 2)]
            cp[x + 5, H : H + J] = black
            acc = place(acc, black, [
                p for h in (0, 1)
                for p in ((h * K, 15 * q + 3 * h, 3), (h * K + K - 3, 61 + 15 * q + 3 * h, 3))
            ])
            for t in (0, 1):
                cd[tile(x, t), H : H + J] = dens[t]
                total = total + dens[t]
                acc = place(acc, dens[t], [
                    p for h in (0, 1) for o in (15 * q + 6 + 4 * t + 2 * h,)
                    for p in ((h * K, o, 2), (h * K + K - 2, 62 + o, 2))
                ])
        z1s[g] = acc
    total = jnp.where(l8 < 2 * K, total, 0.0)

    pl.semaphore_wait(barrier, len(steps) if near else n - 1)
    first = Exchange(0)
    for dx, dy in SIDES:
        if dx or dy:
            edge = dx != 0 and dy != 0
            block(first, cp, cp, part(dx, X, 4 if edge else 5, 5), part(dy, J, 2 if edge else 3, H), (dx, dy, 0))
            block(first, cd, cd, part(dx, 2 * X, 5 if edge else 7, 8), part(dy, J, 2, H), (dx, dy, 0))
        for dz in (1, -1):
            g0, gn, g1 = part(dx, G, 1, 1)
            block(first, z1s, z1r, (g0 - 1, gn, g1), part(dy, J, 2, H), (dx, dy, dz), H, max(dz, 0))
    first.wait()

    def base(x, b):
        return 8 + ((x + 5) * 2 + b) * T

    def get(ref, x, b, off=0):
        return ref[pl.ds(base(x, b) + off, T), :]

    def own(ref, x, b, off=0):
        return ref[pl.ds(base(x, b) + H + off, J), :]

    sides = {}

    def side(x):
        g = x // 4 + 1
        if g not in sides:
            sides[g] = jnp.where(lane[T] < 60, z1r[0, g], z1r[1, g])
        return sides[g]

    for x in range(-5, X + 5):
        far = max(-x, x - X + 1, 0)
        z = side(x) if far < 5 else None
        for h in (0, 1):
            s = 15 * (x % 4) + 3 * h
            B[pl.ds(base(x, h), T), :] = with_sides(cp[x + 5], h, z, K - s, 64 - s)
        for t, ref in ((0, SR), (1, SB)):
            if far <= 4 - t:
                for h in (0, 1):
                    s = 15 * (x % 4) + 6 + 4 * t + 2 * h
                    ref[pl.ds(base(x, h), T), :] = with_sides(cd[tile(x, t)], h, z, K - s, 64 - s)

    sixth = jnp.float32(1.0 / 6.0)

    def beside(read, v, x, b, colour):
        c = (x + b + colour) % 2
        mid = read(v, x, b)
        t = read(v, x - 1, b) + read(v, x + 1, b)
        t = t + (read(v, x, 1 - b) + read(v, x, 1 - b, 2 * b - 1))
        return t + (mid + turn(mid, 1 - 2 * c))

    def half(depth, colour):
        new, old, src = ((R, B, SR), (B, R, SB))[colour]
        for x in range(-depth, X + depth):
            for b in (0, 1):
                new[pl.ds(base(x, b), T), :] = (beside(get, old, x, b, colour) - get(src, x, b)) * sixth

    for k in range(4):
        half(4 - k, k % 2)

    def even_at(rows):
        return (iota(rows, 0) + lane[rows]) % 2 == 0

    even = {rows: even_at(rows) for rows in {J, T}}
    one = []
    for i in range(I):
        left = None
        for x in (2 * i, 2 * i + 1):
            for b in (0, 1):
                for colour, (v, w, s) in enumerate(((R, B, SR), (B, R, SB))):
                    r = own(s, x, b) - (beside(own, w, x, b, colour) - 6.0 * own(v, x, b))
                    left = r if left is None else left + r
        one.append(left * 0.5)
    load_rw.wait()
    sums = [jnp.zeros((J, 128), jnp.float32) for _ in names]
    for g in range(GL):
        acc = jnp.zeros((J, 128), jnp.float32)
        for q in range(3):
            m = 3 * g + q
            red = jnp.where(even[J], one[2 * m], one[2 * m + 1])
            black = jnp.where(even[J], one[2 * m + 1], one[2 * m])
            both = two(red, black)
            if 2 * K < 128:
                both = jnp.where(l8 < 2 * K, both, 0.0)
            cl[E + m, H1 : H1 + J] = both
            sums = [a + rw[f, m] * both for f, a in enumerate(sums)]
            for c, v in enumerate((red, black)):
                s = 18 * q + 9 * c
                acc = place(acc, v, [(0, s, DEEP), (K - DEEP, 55 + s, DEEP)])
        zls[g] = acc

    def stack(rows):
        rows = [jnp.sum(v, axis=0, keepdims=True) for v in rows]
        rows = rows + [jnp.zeros((1, 128), jnp.float32)] * (Q - len(rows))
        return jnp.sum(jnp.concatenate(rows, axis=0), axis=1, keepdims=True)

    spot = lax.broadcasted_iota(jnp.int32, (Q, 128), 0) == lax.broadcasted_iota(jnp.int32, (Q, 128), 1)
    gat[0] = jnp.sum(jnp.where(spot, stack(sums + [total]), 0.0), axis=0, keepdims=True)

    def spread(o, carry):
        if isinstance(o, int):
            there = ((-(o // (ny * nz)) % nx) * ny + -(o // nz) % ny) * nz + -o % nz
        else:
            ox, oy, oz = o // (ny * nz), (o // nz) % ny, o % nz
            there = (lax.rem(nx - ox, nx) * ny + lax.rem(ny - oy, ny)) * nz + lax.rem(nz - oz, nz)
        pltpu.make_async_remote_copy(
            src_ref=gat.at[0], dst_ref=gat.at[there], send_sem=ssem.at[2], recv_sem=rsem.at[2],
            device_id=device(o), device_id_type=MESH,
        ).start()
        return carry

    each_other(spread)

    second = Exchange(1)

    def deep(d, own, count, first):
        if abs(d) < 2:
            return part(d, own, min(own, count), first)
        count -= own
        return (first + own - count, count, first - own - count) if d > 0 else (first, count, first + 2 * own)

    ways = (2, -2, 1, -1, 0)
    for dy in ways:
        for dx in (1, 0) if ring else ways:
            if abs(dx) + abs(dy) > 3 or (abs(dy) == 2 and J >= DEEP) or (abs(dx) == 2 and M >= E):
                continue
            px = (0, M, M if dx else 0) if ring else deep(dx, M, E, E)
            pz = (0, GL, GL * dx) if ring else (0, GL, GL * (2 - dx))
            py = deep(dy, J, DEEP, H1)
            for dz in (1, -1):
                block(second, zls, zlr, pz, py, (dx, dy, dz), H1, max(dz, 0))
            if dx or dy:
                block(second, cl, cl, px, py, (dx, dy, 0))

    for f in range(F):
        acc = jnp.zeros((J, 128), jnp.float32)
        for q in range(FW):
            x = f * FW + q
            v = two(own(B, x, 0), own(B, x, 1))
            cf[x + 4, H : H + J] = v
            acc = place(acc, v, [
                p for h in (0, 1) for o in (4 * q + 2 * h,)
                for p in ((h * K, o, 2), (h * K + K - 2, 62 + o, 2))
            ])
        zfs[f] = acc
    fourth = Exchange(3)
    for dx, dy in SIDES:
        if dx or dy:
            edge = dx != 0 and dy != 0
            block(fourth, cf, cf, part(dx, X, 3 if edge else 4, 4), part(dy, J, 2, H), (dx, dy, 0))
        for dz in (1, -1):
            g0, gn, g1 = part(dx, F, 1, 1)
            block(fourth, zfs, zfr, (g0 - 1, gn, g1), part(dy, J, 2, H), (dx, dy, dz), H, max(dz, 0))

    load_cw.wait()
    others = gat.at[pl.ds(0, n - 1)]
    pltpu.make_async_copy(others, others, rsem.at[2]).wait()
    pltpu.make_async_copy(others, others, ssem.at[2]).wait()
    values = gat[:, 0, :]
    whole = jnp.sum(values, axis=0, keepdims=True)
    values = values - whole / jnp.float32(n)
    lane1 = lax.broadcasted_iota(jnp.int32, (1, 128), 1)
    cv[...] = jnp.broadcast_to(
        stack([cw[o] * values for o in range(NF)] + [jnp.where(lane1 == NF, whole, 0.0)]), (Q, 128)
    )
    mean = cv[NF : NF + 1, :] / jnp.float32(n * X * Y * Z)
    row = iota(T1, 0)
    at = lane[T1]
    maps = {}
    for dx in ((0, 1) if ring else (0, 1, -1)):
        by_row = []
        for dy in (-1, 0, 1):
            vals = [cv[names.index((dx % nx, dy % ny, dz % nz)), :][None] for dz in (-1, 0, 1)]
            by_row.append(jnp.where(at < K, vals[1], jnp.where(at < (K + 128) // 2, vals[2], vals[0])))
        field = jnp.where(row < H1, by_row[0], jnp.where(row < H1 + J, by_row[1], by_row[2]))
        maps[dx] = field + mean * jnp.float32(8.0 / 3.0)

    def base1(m):
        return 8 + ((m % (2 * M)) if ring else m + 6) * T1

    def span(depth):
        low, high = (-depth) // 2, (I - 1 + depth) // 2
        return range(2 * M) if ring and high - low + 1 >= 2 * M else range(low, high + 1)

    def window(depth):
        reach = -(-depth // 4) * 4
        return H1 - reach, J + 2 * reach

    def get1(ref, m, start, rows):
        return ref[pl.ds(base1(m) + start, rows), :]

    second.wait()
    sides.clear()
    for m in span(DEEP):
        g, q = m // 3 + (0 if ring else 2 * GL), m % 3
        if g not in sides:
            sides[g] = jnp.where(lane[T1] < 55, zlr[0, g], zlr[1, g])
        for c, ref in ((0, LR), (1, LB)):
            s = 18 * q + 9 * c
            ref[pl.ds(base1(m), T1), :] = with_sides(cl[m + E], c, sides[g], K - s, 64 - s)

    for m in span(DEEP):
        ER[pl.ds(base1(m), T1), :] = get1(LR, m, 0, T1) * -sixth

    masks = {}

    def even_from(start, rows):
        if rows not in masks:
            masks[rows] = (lax.broadcasted_iota(jnp.int32, (rows, 128), 0) + lax.broadcasted_iota(jnp.int32, (rows, 128), 1)) % 2 == 0
        return masks[rows] if start % 2 == 0 else jnp.logical_not(masks[rows])

    def half1(depth, colour, shift=None, first=False):
        new, old, src = ((ER, EB, LR), (EB, ER, LB))[colour]
        start, rows = window(depth)
        mask = even_from(start, rows)
        for m in span(depth):
            c = get1(old, m, start, rows)
            before, after = get1(old, m - 1, start, rows), get1(old, m + 1, start, rows)
            t = c + (jnp.where(mask, before, after) if colour == 0 else jnp.where(mask, after, before))
            t = t + (get1(old, m, start - 1, rows) + get1(old, m, start + 1, rows))
            t = t + (turn(c, 1) + turn(c, -1)) - get1(src, m, start, rows)
            if shift is not None:
                t = t + shift
            new[pl.ds(base1(m) + start, rows), :] = t * sixth

    half1(8, 1)
    half1(7, 0)
    half1(6, 1)
    for m in span(6):
        dx = (0 if 0 <= m < M else 1) if ring else (-1 if m < 0 else (0 if m < M else 1))
        start, rows = window(6)
        EB[pl.ds(base1(m) + start, rows), :] = get1(EB, m, start, rows) + maps[dx][start : start + rows]
    shift = 4.0 * mean
    half1(5, 0, shift)
    half1(4, 1, shift)
    half1(3, 0, shift)
    half1(2, 1, shift)

    fourth.wait()
    sides.clear()
    rise = mean * jnp.float32(2.0 / 3.0)
    for m in range(-1, M + 1):
        tiles = [get1(v, m, H1 - H, T) for v in (ER, EB)]
        for i in (2 * m, 2 * m + 1):
            first_, second_ = tiles if i % 2 == 0 else tiles[::-1]
            e = jnp.where(even[T], first_, second_) + rise
            for x in (2 * i, 2 * i + 1):
                far = max(-x, x - X + 1, 0)
                z = None
                if far < 4:
                    f = 0 if x < 0 else (F + 1 if x >= X else x // FW + 1)
                    if f not in sides:
                        sides[f] = jnp.where(lane[T] < 60, zfr[0, f], zfr[1, f])
                    z = sides[f]
                for h in (0, 1):
                    s = 4 * (x % FW) + 2 * h
                    B[pl.ds(base(x, h), T), :] = with_sides(cf[x + 4], h, z, K - s, 64 - s) + e

    def last(depth, colour):
        new, old, src = ((R, B, SR), (B, R, SB))[colour]
        for x in range(-depth, X + depth):
            for b in (0, 1):
                t = beside(get, old, x, b, colour) - get(src, x, b) + mean
                new[pl.ds(base(x, b), T), :] = t * sixth

    last(3, 0)
    last(2, 1)
    last(1, 0)
    back = l8 >> 1
    odd_lane = (l8 & 1) == 1
    for x in range(X):
        for b in (0, 1):
            red = own(R, x, b)
            dark = (beside(own, R, x, b, 1) - own(SB, x, b) + mean) * sixth
            pair = (red, dark) if (x + b) % 2 == 0 else (dark, red)
            e, o = (jnp.take_along_axis(v, back, axis=1, mode="promise_in_bounds") for v in pair)
            out_ref[x, pl.ds(b, J, stride=2), :] = jnp.where(odd_lane, o, e)[:, 0:Z]


def body(dims, density, potential):
    nx, ny, nz, X, Y, Z = dims
    n = nx * ny * nz
    I, J, K = X // 2, Y // 2, Z // 2
    T, T1 = J + 2 * H, J + 2 * H1
    M = I // 2
    ring = nx == 2 and I < DEEP
    G, F, GL = X // 4, max(X // 12, 1), M // 3
    op = coarse_operator(nx, ny, nz, float(J * K), float(I * K), float(I * J))
    rw = residual_weights(nx, ny, nz, I, J, K)
    cw = coarse_weights(op, nx, ny, nz)
    Q = -(-(len(rw) + 1) // 8) * 8
    fine = 16 + (X + 10) * 2 * T
    coarse = 16 + (2 * M if ring else M + 12) * T1

    def vmem(*shape):
        return pltpu.VMEM(shape, jnp.float32)

    return pl.pallas_call(
        functools.partial(kernel, dims),
        out_shape=pltpu.VMEM((X, Y, Z), jnp.float32),
        in_specs=[pl.BlockSpec(memory_space=pl.ANY)] * 4,
        out_specs=pl.BlockSpec(memory_space=pltpu.VMEM),
        scratch_shapes=[
            vmem(X, Y, 128),
            vmem(X, Y, 128),
            vmem(*rw.shape),
            vmem(*cw.shape),
            vmem(X + 10, T, 128),
            vmem(2 * (X + 8), T, 128),
            vmem(X + 8, T, 128),
            vmem(2 * M if ring else M + 10, T1, 128),
            vmem(G, J, 128),
            vmem(2, G + 2, T, 128),
            vmem(F, J, 128),
            vmem(2, F + 2, T, 128),
            vmem(GL, J, 128),
            vmem(2, (2 if ring else 5) * GL, T1, 128),
            vmem(fine, 128),
            vmem(fine, 128),
            vmem(fine, 128),
            vmem(fine, 128),
            vmem(coarse, 128),
            vmem(coarse, 128),
            vmem(coarse, 128),
            vmem(coarse, 128),
            vmem(n, 1, 128),
            vmem(Q, 128),
            vmem(2048, 128),
            pltpu.SemaphoreType.DMA((4,)),
            pltpu.SemaphoreType.DMA((4,)),
            pltpu.SemaphoreType.DMA((4,)),
        ],
        compiler_params=pltpu.CompilerParams(collective_id=0, has_side_effects=True),
        name="vcycle",
    )(density, potential, rw, cw)


def solution(mesh):
    nx, ny, nz = (mesh.shape[a] for a in ("gx", "gy", "gz"))

    def run(density, potential):
        return body((nx, ny, nz) + density.shape, density, potential)

    spec = P("gx", "gy", "gz")
    return jax.shard_map(run, mesh=mesh, in_specs=(spec, spec), out_specs=spec, check_vma=False)
```

```python
import functools
import numpy as np
import jax
import jax.numpy as jnp
from jax import lax
from jax.experimental import pallas as pl
from jax.experimental.pallas import tpu as pltpu
from jax.sharding import PartitionSpec as P

HI = lax.Precision.HIGHEST
MESH = pl.DeviceIdType.MESH
H, H1 = 4, 12
DEEP = 9
A, B_, AA, BB = 1, -1, 2, -2
SIDES = ((1, A), (-1, A), (0, A), (1, B_), (-1, B_), (0, B_), (0, 0), (1, 0), (-1, 0))


def table(count):
    modes = (np.arange(count) + 1) // 2
    angle = 2 * np.pi * np.outer(np.arange(count), modes) / count
    q = np.where(np.arange(count) % 2 == 1, np.cos(angle), np.sin(angle)) * np.sqrt(2 / count)
    q = np.where(2 * modes == count, np.cos(angle) / np.sqrt(count), q)
    q[:, 0] = 1 / np.sqrt(count)
    return q, 2 - 2 * np.cos(2 * np.pi * modes / count)


def coarse_operator(nx, ny, nz, wx, wy, wz):
    qx, lx = table(nx)
    qy, ly = table(ny)
    qz, lz = table(nz)
    q = np.kron(np.kron(qx, qy), qz)
    lam = wx * lx[:, None, None] + wy * ly[None, :, None] + wz * lz[None, None, :]
    lam = lam.reshape(-1)
    inv = np.concatenate([[0.0], -1.0 / lam[1:]])
    return ((q * inv) @ q.T).astype(np.float32)


def offsets(nx, ny, nz):
    steps = [(dx % nx, dy % ny, dz % nz) for dx in (0, 1, -1) for dy in (0, 1, -1) for dz in (0, 1, -1)]
    return list(dict.fromkeys(steps))


def residual_weights(nx, ny, nz, I, J, K):
    block = np.zeros((3 * I, 3 * J, 3 * K))
    block[I : 2 * I, J : 2 * J, K : 2 * K] = 1.0

    def beside(v):
        return sum(np.roll(v, d, axis) for axis in range(3) for d in (1, -1))

    red = np.indices(block.shape).sum(0) % 2 == 0
    v = beside(block) - 6.0 * block
    black2 = np.where(red, 0.0, v)
    red2 = np.where(red, v + beside(black2) / 6.0, 0.0)
    black1 = np.where(red, 0.0, beside(red2) / 6.0)
    red1 = np.where(red, beside(black1) / 6.0, 0.0)
    w = block + (black2 + red2 + black1 + red1) / 6.0
    names = offsets(nx, ny, nz)
    own = np.zeros((len(names), I, J, K))
    for dx in (0, 1, -1):
        for dy in (0, 1, -1):
            for dz in (0, 1, -1):
                x, y, z = (1 - dx) * I, (1 - dy) * J, (1 - dz) * K
                own[names.index((dx % nx, dy % ny, dz % nz))] += w[x : x + I, y : y + J, z : z + K]
    even = np.indices((J, K)).sum(0) % 2 == 0
    first, second = own[:, 0::2], own[:, 1::2]
    out = np.zeros((len(names), I // 2, J, 128))
    out[..., :K] = np.where(even, first, second)
    out[..., K : 2 * K] = np.where(even, second, first)
    return out.astype(np.float32)


def coarse_weights(op, nx, ny, nz):
    names = offsets(nx, ny, nz)
    green = op.astype(np.float64)[:, 0].reshape(nx, ny, nz)
    rx, ry, rz = np.indices((nx, ny, nz)).reshape(3, -1)
    out = np.zeros((len(names), nx * ny * nz, 128))
    for o, (ox, oy, oz) in enumerate(names):
        for f, (fx, fy, fz) in enumerate(names):
            out[o, :, f] = green[(ox - rx - fx) % nx, (oy - ry - fy) % ny, (oz - rz - fz) % nz]
    return out.astype(np.float32)


def turn(v, shift):
    shift %= 128
    return pltpu.roll(v, shift, 1) if shift else v


def kernel(
    dims, den_hbm, pot_hbm, rw_hbm, cw_hbm, out_ref,
    den_v, pot_v, rw, cw, cp, cd, cf, cl,
    z1s, z1r, zfs, zfr, zls, zlr,
    R, B, SR, SB, LR, LB, ER, EB, gat, cv, dummy,
    ssem, rsem, lsem,
):
    nx, ny, nz, X, Y, Z = dims
    n = nx * ny * nz
    I, J, K = X // 2, Y // 2, Z // 2
    T, T1 = J + 2 * H, J + 2 * H1
    M = I // 2
    ring = nx == 2 and I < DEEP
    E = 0 if ring else 5
    G, F, GL = X // 4, max(X // 12, 1), M // 3
    FW = X // F
    assert X % 12 == 0 and FW <= 12 and 2 * K <= 128 and J % 8 == 0 and 2 * J > DEEP and 2 * M >= E and M % 3 == 0
    names = offsets(nx, ny, nz)
    NF = len(names)
    Q = -(-(NF + 1) // 8) * 8
    ix, iy, iz = lax.axis_index("gx"), lax.axis_index("gy"), lax.axis_index("gz")
    me = (ix * ny + iy) * nz + iz

    def around(i, count):
        return [i] + [jnp.where(i + o >= count, i + o - count, i + o) for o in range(1, count)]

    xs, ys, zs = around(ix, nx), around(iy, ny), around(iz, nz)

    def device(o):
        if isinstance(o, int):
            return (xs[o // (ny * nz)], ys[o // nz % ny], zs[o % nz])
        ox, oy, oz = o // (ny * nz), (o // nz) % ny, o % nz
        return (lax.rem(ix + ox, nx), lax.rem(iy + oy, ny), lax.rem(iz + oz, nz))

    def each_other(step):
        if n <= 64:
            for o in range(1, n):
                step(o, 0)
        else:
            lax.fori_loop(1, n, step, 0)

    wide = (lambda ref: ref) if Z == 128 else (lambda ref: ref.at[:, :, pl.ds(0, Z)])
    load_p = pltpu.make_async_copy(pot_hbm, wide(pot_v), lsem.at[0])
    load_d = pltpu.make_async_copy(den_hbm, wide(den_v), lsem.at[1])
    load_rw = pltpu.make_async_copy(rw_hbm, rw, lsem.at[2])
    load_cw = pltpu.make_async_copy(cw_hbm, cw, lsem.at[3])
    load_p.start()
    load_d.start()
    load_rw.start()
    load_cw.start()

    barrier = pltpu.get_barrier_semaphore()

    def greet(o, carry):
        pl.semaphore_signal(barrier, inc=1, device_id=device(o), device_id_type=MESH)
        return carry

    near = max(nx, ny, nz) <= 5
    steps = sorted({
        (dx % nx * ny + dy % ny) * nz + dz % nz
        for dx in (-1, 0, 1) for dy in (-1, 0, 1) for dz in (-1, 0, 1)
    } - {0})
    if near:
        for o in steps:
            greet(o, 0)
    else:
        each_other(greet)
    up = {1: iy > 0, -1: iy == 0}

    def along_y(d):
        if d == 0:
            return iy
        return jnp.where(up[1 if d > 0 else -1], ys[abs(d)], ys[-abs(d)])

    target_y = {d: along_y(d) for d in (0, 1, -1) + ((2, -2) if ny > 2 else ())}

    def part_y(d, own, count, first, low=None, high=None):
        if d == 0:
            return first, own, first
        low = first - count if low is None else low
        high = first + own if high is None else high
        goes_up = up[1 if d > 0 else -1]
        return jnp.where(goes_up, first + own - count, first), count, jnp.where(goes_up, low, high)

    class Exchange:
        def __init__(self, k):
            self.k, self.rows = k, 0

        def send(self, src, dst, at, to):
            dx, dy, dz = to
            copy = pltpu.make_async_remote_copy(
                src_ref=src, dst_ref=dst, send_sem=ssem.at[self.k], recv_sem=rsem.at[self.k],
                device_id=(xs[dx], target_y[dy], zs[dz]), device_id_type=MESH,
            )
            copy.start()
            self.rows += at

        def wait(self):
            all_of = dummy.at[pl.ds(0, self.rows)]
            pltpu.make_async_copy(all_of, all_of, rsem.at[self.k]).wait()
            pltpu.make_async_copy(all_of, all_of, ssem.at[self.k]).wait()

    def part(d, own, count, first):
        if d == 0:
            return first, own, first
        if d == 1:
            return first + own - count, count, first - count
        return first, count, first + own

    def block(ex, src, dst, px, py, to, shift=0, lead=None):
        (sx, cx, tx), (sy, cy, ty) = px, py
        target = dst if lead is None else dst.at[lead]
        ex.send(
            src.at[pl.ds(sx, cx), pl.ds(sy - shift, cy)],
            target.at[pl.ds(tx, cx), pl.ds(ty, cy)],
            cx * cy, to,
        )

    def iota(rows, dim):
        return lax.broadcasted_iota(jnp.int32, (rows, 128), dim)

    lane = {rows: iota(rows, 1) for rows in {J, T, T1}}

    def place(acc, v, pieces):
        by_shift = {}
        for src, dst, width in pieces:
            by_shift.setdefault((dst - src) % 128, []).append((dst, width))
        at = lane[v.shape[0]]
        for shift, spans in by_shift.items():
            mask = None
            for dst, width in spans:
                inside = (at >= dst) & (at < dst + width)
                mask = inside if mask is None else mask | inside
            moved = turn(v, shift)
            acc = jnp.where(mask, moved, acc)
        return acc

    def outside(z, right, left):
        if (right - left) % 128 == 0:
            return turn(z, right)
        return jnp.where(lane[z.shape[0]] < 96, turn(z, right), turn(z, left))

    def with_sides(v, half, z, right, left):
        own = turn(v, -K) if half else v
        if z is None:
            return own
        return jnp.where(lane[v.shape[0]] < K, own, outside(z, right, left))

    def two(a, b):
        return jnp.where(lane[a.shape[0]] < K, a, turn(b, K))

    l8 = lane[J]
    low = jnp.where(l8 < K, 2 * l8, 2 * (l8 - K) + 1) & 127
    high = jnp.where(l8 < K, 2 * l8 + 1, 2 * (l8 - K)) & 127
    order = (low, high)

    def colours(ref, x, which):
        v = [ref[x, pl.ds(b, J, stride=2), :] for b in (0, 1)]
        take = [jnp.take_along_axis(u, order[which], axis=1, mode="promise_in_bounds") for u in v]
        return jnp.where(l8 < K, take[0], take[1])

    def tile(x, t):
        forward = 0 <= x < X // 2 or x >= X
        return 2 * (x + 4) + (t if forward else 1 - t)

    load_p.wait()
    load_d.wait()
    total = jnp.zeros((J, 128), jnp.float32)
    for g in range(G):
        acc = jnp.zeros((J, 128), jnp.float32)
        for q in range(4):
            x = 4 * g + q
            black = colours(pot_v, x, 1 - x % 2)
            dens = [colours(den_v, x, x % 2), colours(den_v, x, 1 - x % 2)]
            cp[x + 5, H : H + J] = black
            acc = place(acc, black, [
                p for h in (0, 1)
                for p in ((h * K, 15 * q + 3 * h, 3), (h * K + K - 3, 61 + 15 * q + 3 * h, 3))
            ])
            for t in (0, 1):
                cd[tile(x, t), H : H + J] = dens[t]
                total = total + dens[t]
                acc = place(acc, dens[t], [
                    p for h in (0, 1) for o in (15 * q + 6 + 4 * t + 2 * h,)
                    for p in ((h * K, o, 2), (h * K + K - 2, 62 + o, 2))
                ])
        z1s[g] = acc
    total = jnp.where(l8 < 2 * K, total, 0.0)

    pl.semaphore_wait(barrier, len(steps) if near else n - 1)
    first = Exchange(0)

    def trim(ex, dx, src, dst, own, at, steps, py, to):
        seen = 0
        for count, rows in steps:
            px = (at + own - seen - count, count, at - seen - count) if dx == 1 else (at + seen, count, at + own + seen)
            block(ex, src, dst, px, py(rows), to)
            seen += count

    def send_y(dy):
        for dx in (1, -1, 0):
            to = (dx, dy, 0)
            if dx:
                trim(first, dx, cp, cp, X, 5, ((2, 2), (2, 1)), lambda rows: part_y(dy, J, rows, H), to)
                trim(first, dx, cd, cd, 2 * X, 8, ((2, 2), (3, 1)), lambda rows: part_y(dy, J, rows, H), to)
            else:
                block(first, cp, cp, (5, X, 5), part_y(dy, J, 3, H), to)
                block(first, cd, cd, (8, 2 * X, 8), part_y(dy, J, 2, H), to)
            for dz in (1, -1):
                g0, gn, g1 = part(dx, G, 1, 1)
                block(first, z1s, z1r, (g0 - 1, gn, g1), part_y(dy, J, 2, H), (dx, dy, dz), H, max(dz, 0))

    send_y(A)
    send_y(B_)
    for dx in (0, 1, -1):
        for dz in (1, -1):
            g0, gn, g1 = part(dx, G, 1, 1)
            block(first, z1s, z1r, (g0 - 1, gn, g1), (H, J, H), (dx, 0, dz), H, max(dz, 0))
        if dx:
            block(first, cp, cp, part(dx, X, 5, 5), (H, J, H), (dx, 0, 0))
            block(first, cd, cd, part(dx, 2 * X, 7, 8), (H, J, H), (dx, 0, 0))
    first.wait()

    def base(x, b):
        return 8 + ((x + 5) * 2 + b) * T

    def get(ref, x, b, off=0):
        return ref[pl.ds(base(x, b) + off, T), :]

    def own(ref, x, b, off=0):
        return ref[pl.ds(base(x, b) + H + off, J), :]

    sides = {}

    def side(x):
        g = x // 4 + 1
        if g not in sides:
            sides[g] = jnp.where(lane[T] < 60, z1r[0, g], z1r[1, g])
        return sides[g]

    for x in range(-5, X + 5):
        far = max(-x, x - X + 1, 0)
        z = side(x) if far < 5 else None
        for h in (0, 1):
            s = 15 * (x % 4) + 3 * h
            B[pl.ds(base(x, h), T), :] = with_sides(cp[x + 5], h, z, K - s, 64 - s)
        for t, ref in ((0, SR), (1, SB)):
            if far <= 4 - t:
                for h in (0, 1):
                    s = 15 * (x % 4) + 6 + 4 * t + 2 * h
                    ref[pl.ds(base(x, h), T), :] = with_sides(cd[tile(x, t)], h, z, K - s, 64 - s)

    sixth = jnp.float32(1.0 / 6.0)

    def beside(read, v, x, b, colour):
        c = (x + b + colour) % 2
        mid = read(v, x, b)
        t = read(v, x - 1, b) + read(v, x + 1, b)
        t = t + (read(v, x, 1 - b) + read(v, x, 1 - b, 2 * b - 1))
        return t + (mid + turn(mid, 1 - 2 * c))

    def half(depth, colour):
        new, old, src = ((R, B, SR), (B, R, SB))[colour]
        for x in range(-depth, X + depth):
            for b in (0, 1):
                new[pl.ds(base(x, b), T), :] = (beside(get, old, x, b, colour) - get(src, x, b)) * sixth

    for k in range(4):
        half(4 - k, k % 2)

    def even_at(rows):
        return (iota(rows, 0) + lane[rows]) % 2 == 0

    even = {rows: even_at(rows) for rows in {J, T}}
    one = []
    for i in range(I):
        left = None
        for x in (2 * i, 2 * i + 1):
            for b in (0, 1):
                for colour, (v, w, s) in enumerate(((R, B, SR), (B, R, SB))):
                    r = own(s, x, b) - (beside(own, w, x, b, colour) - 6.0 * own(v, x, b))
                    left = r if left is None else left + r
        one.append(left * 0.5)
    load_rw.wait()
    sums = [jnp.zeros((J, 128), jnp.float32) for _ in names]
    for g in range(GL):
        acc = jnp.zeros((J, 128), jnp.float32)
        for q in range(3):
            m = 3 * g + q
            red = jnp.where(even[J], one[2 * m], one[2 * m + 1])
            black = jnp.where(even[J], one[2 * m + 1], one[2 * m])
            both = two(red, black)
            if 2 * K < 128:
                both = jnp.where(l8 < 2 * K, both, 0.0)
            cl[E + m, H1 : H1 + J] = both
            sums = [a + rw[f, m] * both for f, a in enumerate(sums)]
            for c, v in enumerate((red, black)):
                s = 18 * q + 9 * c
                acc = place(acc, v, [(0, s, DEEP), (K - DEEP, 55 + s, DEEP)])
        zls[g] = acc

    def stack(rows):
        rows = [jnp.sum(v, axis=0, keepdims=True) for v in rows]
        rows = rows + [jnp.zeros((1, 128), jnp.float32)] * (Q - len(rows))
        return jnp.sum(jnp.concatenate(rows, axis=0), axis=1, keepdims=True)

    spot = lax.broadcasted_iota(jnp.int32, (Q, 128), 0) == lax.broadcasted_iota(jnp.int32, (Q, 128), 1)
    gat[0] = jnp.sum(jnp.where(spot, stack(sums + [total]), 0.0), axis=0, keepdims=True)

    def spread(o, carry):
        if isinstance(o, int):
            there = ((-(o // (ny * nz)) % nx) * ny + -(o // nz) % ny) * nz + -o % nz
        else:
            ox, oy, oz = o // (ny * nz), (o // nz) % ny, o % nz
            there = (lax.rem(nx - ox, nx) * ny + lax.rem(ny - oy, ny)) * nz + lax.rem(nz - oz, nz)
        pltpu.make_async_remote_copy(
            src_ref=gat.at[0], dst_ref=gat.at[there], send_sem=ssem.at[2], recv_sem=rsem.at[2],
            device_id=device(o), device_id_type=MESH,
        ).start()
        return carry

    each_other(spread)

    second = Exchange(1)

    def deep(d, own, count, first):
        if abs(d) < 2:
            return part(d, own, min(own, count), first)
        count -= own
        return (first + own - count, count, first - own - count) if d > 0 else (first, count, first + 2 * own)

    def deep_y(d, own, count, first):
        if abs(d) < 2:
            return part_y(d, own, min(own, count), first)
        count -= own
        return part_y(d, own, count, first, first - own - count, first + 2 * own)

    for dy in (AA, BB, A, B_, 0):
        for dx in (1, 0) if ring else (1, -1, 0, 2, -2):
            if abs(dx) + abs(dy) > 3 or (abs(dy) == 2 and J >= DEEP) or (abs(dx) == 2 and M >= E):
                continue
            px = (0, M, M if dx else 0) if ring else deep(dx, M, E, E)
            pz = (0, GL, GL * dx) if ring else (0, GL, GL * (2 - dx))
            py = deep_y(dy, J, DEEP, H1)
            for dz in (1, -1):
                block(second, zls, zlr, pz, py, (dx, dy, dz), H1, max(dz, 0))
            if dx or dy:
                block(second, cl, cl, px, py, (dx, dy, 0))

    for f in range(F):
        acc = jnp.zeros((J, 128), jnp.float32)
        for q in range(FW):
            x = f * FW + q
            v = two(own(B, x, 0), own(B, x, 1))
            cf[x + 4, H : H + J] = v
            acc = place(acc, v, [
                p for h in (0, 1) for o in (4 * q + 2 * h,)
                for p in ((h * K, o, 2), (h * K + K - 2, 62 + o, 2))
            ])
        zfs[f] = acc
    fourth = Exchange(3)
    twice = nx == 2 and F == 1
    for dx, dy in SIDES:
        to = (dx, dy, 0)
        if dx and dy:
            trim(fourth, dx, cf, cf, X, 4, ((1, 2), (2, 1)), lambda rows: part_y(dy, J, rows, H), to)
        elif dx or dy:
            block(fourth, cf, cf, part(dx, X, 4, 4), part_y(dy, J, 2, H), to)
        if dx == -1 and twice:
            continue
        for dz in (1, -1):
            g0, gn, g1 = part(dx, F, 1, 1)
            block(fourth, zfs, zfr, (g0 - 1, gn, g1), part_y(dy, J, 2, H), (dx, dy, dz), H, max(dz, 0))

    load_cw.wait()
    others = gat.at[pl.ds(0, n - 1)]
    pltpu.make_async_copy(others, others, rsem.at[2]).wait()
    pltpu.make_async_copy(others, others, ssem.at[2]).wait()
    values = gat[:, 0, :]
    whole = jnp.sum(values, axis=0, keepdims=True)
    values = values - whole / jnp.float32(n)
    lane1 = lax.broadcasted_iota(jnp.int32, (1, 128), 1)
    cv[...] = jnp.broadcast_to(
        stack([cw[o] * values for o in range(NF)] + [jnp.where(lane1 == NF, whole, 0.0)]), (Q, 128)
    )
    mean = cv[NF : NF + 1, :] / jnp.float32(n * X * Y * Z)
    row = iota(T1, 0)
    at = lane[T1]
    maps = {}
    for dx in ((0, 1) if ring else (0, 1, -1)):
        by_row = []
        for dy in (-1, 0, 1):
            vals = [cv[names.index((dx % nx, dy % ny, dz % nz)), :][None] for dz in (-1, 0, 1)]
            by_row.append(jnp.where(at < K, vals[1], jnp.where(at < (K + 128) // 2, vals[2], vals[0])))
        field = jnp.where(row < H1, by_row[0], jnp.where(row < H1 + J, by_row[1], by_row[2]))
        maps[dx] = field + mean * jnp.float32(8.0 / 3.0)

    def base1(m):
        return 8 + ((m % (2 * M)) if ring else m + 6) * T1

    def span(depth):
        low, high = (-depth) // 2, (I - 1 + depth) // 2
        return range(2 * M) if ring and high - low + 1 >= 2 * M else range(low, high + 1)

    def window(depth):
        reach = -(-depth // 4) * 4
        return H1 - reach, J + 2 * reach

    def get1(ref, m, start, rows):
        return ref[pl.ds(base1(m) + start, rows), :]

    second.wait()
    sides.clear()
    for m in span(DEEP):
        g, q = m // 3 + (0 if ring else 2 * GL), m % 3
        if g not in sides:
            sides[g] = jnp.where(lane[T1] < 55, zlr[0, g], zlr[1, g])
        for c, ref in ((0, LR), (1, LB)):
            s = 18 * q + 9 * c
            ref[pl.ds(base1(m), T1), :] = with_sides(cl[m + E], c, sides[g], K - s, 64 - s)

    for m in span(DEEP):
        ER[pl.ds(base1(m), T1), :] = get1(LR, m, 0, T1) * -sixth

    masks = {}

    def even_from(start, rows):
        if rows not in masks:
            masks[rows] = (lax.broadcasted_iota(jnp.int32, (rows, 128), 0) + lax.broadcasted_iota(jnp.int32, (rows, 128), 1)) % 2 == 0
        return masks[rows] if start % 2 == 0 else jnp.logical_not(masks[rows])

    def half1(depth, colour, shift=None, first=False):
        new, old, src = ((ER, EB, LR), (EB, ER, LB))[colour]
        start, rows = window(depth)
        mask = even_from(start, rows)
        for m in span(depth):
            c = get1(old, m, start, rows)
            before, after = get1(old, m - 1, start, rows), get1(old, m + 1, start, rows)
            t = c + (jnp.where(mask, before, after) if colour == 0 else jnp.where(mask, after, before))
            t = t + (get1(old, m, start - 1, rows) + get1(old, m, start + 1, rows))
            t = t + (turn(c, 1) + turn(c, -1)) - get1(src, m, start, rows)
            if shift is not None:
                t = t + shift
            new[pl.ds(base1(m) + start, rows), :] = t * sixth

    half1(8, 1)
    half1(7, 0)
    half1(6, 1)
    for m in span(6):
        dx = (0 if 0 <= m < M else 1) if ring else (-1 if m < 0 else (0 if m < M else 1))
        start, rows = window(6)
        EB[pl.ds(base1(m) + start, rows), :] = get1(EB, m, start, rows) + maps[dx][start : start + rows]
    shift = 4.0 * mean
    half1(5, 0, shift)
    half1(4, 1, shift)
    half1(3, 0, shift)
    half1(2, 1, shift)

    fourth.wait()
    sides.clear()
    rise = mean * jnp.float32(2.0 / 3.0)
    for m in range(-1, M + 1):
        tiles = [get1(v, m, H1 - H, T) for v in (ER, EB)]
        for i in (2 * m, 2 * m + 1):
            first_, second_ = tiles if i % 2 == 0 else tiles[::-1]
            e = jnp.where(even[T], first_, second_) + rise
            for x in (2 * i, 2 * i + 1):
                far = max(-x, x - X + 1, 0)
                z = None
                if far < 4:
                    f = 0 if x < 0 or (x >= X and twice) else (F + 1 if x >= X else x // FW + 1)
                    if f not in sides:
                        sides[f] = jnp.where(lane[T] < 60, zfr[0, f], zfr[1, f])
                    z = sides[f]
                for h in (0, 1):
                    s = 4 * (x % FW) + 2 * h
                    B[pl.ds(base(x, h), T), :] = with_sides(cf[x + 4], h, z, K - s, 64 - s) + e

    def last(depth, colour):
        new, old, src = ((R, B, SR), (B, R, SB))[colour]
        for x in range(-depth, X + depth):
            for b in (0, 1):
                t = beside(get, old, x, b, colour) - get(src, x, b) + mean
                new[pl.ds(base(x, b), T), :] = t * sixth

    last(3, 0)
    last(2, 1)
    last(1, 0)
    back = l8 >> 1
    odd_lane = (l8 & 1) == 1
    for x in range(X):
        for b in (0, 1):
            red = own(R, x, b)
            dark = (beside(own, R, x, b, 1) - own(SB, x, b) + mean) * sixth
            pair = (red, dark) if (x + b) % 2 == 0 else (dark, red)
            e, o = (jnp.take_along_axis(v, back, axis=1, mode="promise_in_bounds") for v in pair)
            out_ref[x, pl.ds(b, J, stride=2), :] = jnp.where(odd_lane, o, e)[:, 0:Z]


def body(dims, density, potential):
    nx, ny, nz, X, Y, Z = dims
    n = nx * ny * nz
    I, J, K = X // 2, Y // 2, Z // 2
    T, T1 = J + 2 * H, J + 2 * H1
    M = I // 2
    ring = nx == 2 and I < DEEP
    G, F, GL = X // 4, max(X // 12, 1), M // 3
    op = coarse_operator(nx, ny, nz, float(J * K), float(I * K), float(I * J))
    rw = residual_weights(nx, ny, nz, I, J, K)
    cw = coarse_weights(op, nx, ny, nz)
    Q = -(-(len(rw) + 1) // 8) * 8
    fine = 16 + (X + 10) * 2 * T
    coarse = 16 + (2 * M if ring else M + 12) * T1

    def vmem(*shape):
        return pltpu.VMEM(shape, jnp.float32)

    return pl.pallas_call(
        functools.partial(kernel, dims),
        out_shape=pltpu.VMEM((X, Y, Z), jnp.float32),
        in_specs=[pl.BlockSpec(memory_space=pl.ANY)] * 4,
        out_specs=pl.BlockSpec(memory_space=pltpu.VMEM),
        scratch_shapes=[
            vmem(X, Y, 128),
            vmem(X, Y, 128),
            vmem(*rw.shape),
            vmem(*cw.shape),
            vmem(X + 10, T, 128),
            vmem(2 * (X + 8), T, 128),
            vmem(X + 8, T, 128),
            vmem(2 * M if ring else M + 10, T1, 128),
            vmem(G, J, 128),
            vmem(2, G + 2, T, 128),
            vmem(F, J, 128),
            vmem(2, F + 2, T, 128),
            vmem(GL, J, 128),
            vmem(2, (2 if ring else 5) * GL, T1, 128),
            vmem(fine, 128),
            vmem(fine, 128),
            vmem(fine, 128),
            vmem(fine, 128),
            vmem(coarse, 128),
            vmem(coarse, 128),
            vmem(coarse, 128),
            vmem(coarse, 128),
            vmem(n, 1, 128),
            vmem(Q, 128),
            vmem(2048, 128),
            pltpu.SemaphoreType.DMA((4,)),
            pltpu.SemaphoreType.DMA((4,)),
            pltpu.SemaphoreType.DMA((4,)),
        ],
        compiler_params=pltpu.CompilerParams(collective_id=0, has_side_effects=True),
        name="vcycle",
    )(density, potential, rw, cw)


def solution(mesh):
    nx, ny, nz = (mesh.shape[a] for a in ("gx", "gy", "gz"))

    def run(density, potential):
        return body((nx, ny, nz) + density.shape, density, potential)

    spec = P("gx", "gy", "gz")
    return jax.shard_map(run, mesh=mesh, in_specs=(spec, spec), out_specs=spec, check_vma=False)
```

```python
import functools
import numpy as np
import jax
import jax.numpy as jnp
from jax import lax
from jax.experimental import pallas as pl
from jax.experimental.pallas import tpu as pltpu
from jax.sharding import PartitionSpec as P

HI = lax.Precision.HIGHEST
MESH = pl.DeviceIdType.MESH
H, H1 = 4, 12
DEEP = 9
A, B_, AA, BB = 1, -1, 2, -2
SIDES = ((1, A), (-1, A), (0, A), (1, B_), (-1, B_), (0, B_), (0, 0), (1, 0), (-1, 0))


def table(count):
    modes = (np.arange(count) + 1) // 2
    angle = 2 * np.pi * np.outer(np.arange(count), modes) / count
    q = np.where(np.arange(count) % 2 == 1, np.cos(angle), np.sin(angle)) * np.sqrt(2 / count)
    q = np.where(2 * modes == count, np.cos(angle) / np.sqrt(count), q)
    q[:, 0] = 1 / np.sqrt(count)
    return q, 2 - 2 * np.cos(2 * np.pi * modes / count)


def coarse_operator(nx, ny, nz, wx, wy, wz):
    qx, lx = table(nx)
    qy, ly = table(ny)
    qz, lz = table(nz)
    q = np.kron(np.kron(qx, qy), qz)
    lam = wx * lx[:, None, None] + wy * ly[None, :, None] + wz * lz[None, None, :]
    lam = lam.reshape(-1)
    inv = np.concatenate([[0.0], -1.0 / lam[1:]])
    return ((q * inv) @ q.T).astype(np.float32)


def offsets(nx, ny, nz):
    steps = [(dx % nx, dy % ny, dz % nz) for dx in (0, 1, -1) for dy in (0, 1, -1) for dz in (0, 1, -1)]
    return list(dict.fromkeys(steps))


def residual_weights(nx, ny, nz, I, J, K):
    block = np.zeros((3 * I, 3 * J, 3 * K))
    block[I : 2 * I, J : 2 * J, K : 2 * K] = 1.0

    def beside(v):
        return sum(np.roll(v, d, axis) for axis in range(3) for d in (1, -1))

    red = np.indices(block.shape).sum(0) % 2 == 0
    v = beside(block) - 6.0 * block
    black2 = np.where(red, 0.0, v)
    red2 = np.where(red, v + beside(black2) / 6.0, 0.0)
    black1 = np.where(red, 0.0, beside(red2) / 6.0)
    red1 = np.where(red, beside(black1) / 6.0, 0.0)
    w = block + (black2 + red2 + black1 + red1) / 6.0
    names = offsets(nx, ny, nz)
    own = np.zeros((len(names), I, J, K))
    for dx in (0, 1, -1):
        for dy in (0, 1, -1):
            for dz in (0, 1, -1):
                x, y, z = (1 - dx) * I, (1 - dy) * J, (1 - dz) * K
                own[names.index((dx % nx, dy % ny, dz % nz))] += w[x : x + I, y : y + J, z : z + K]
    even = np.indices((J, K)).sum(0) % 2 == 0
    first, second = own[:, 0::2], own[:, 1::2]
    out = np.zeros((len(names), I // 2, J, 128))
    out[..., :K] = np.where(even, first, second)
    out[..., K : 2 * K] = np.where(even, second, first)
    return out.astype(np.float32)


def coarse_weights(op, nx, ny, nz):
    names = offsets(nx, ny, nz)
    green = op.astype(np.float64)[:, 0].reshape(nx, ny, nz)
    rx, ry, rz = np.indices((nx, ny, nz)).reshape(3, -1)
    out = np.zeros((len(names), nx * ny * nz, 128))
    for o, (ox, oy, oz) in enumerate(names):
        for f, (fx, fy, fz) in enumerate(names):
            out[o, :, f] = green[(ox - rx - fx) % nx, (oy - ry - fy) % ny, (oz - rz - fz) % nz]
    return out.astype(np.float32)


def turn(v, shift):
    shift %= 128
    return pltpu.roll(v, shift, 1) if shift else v


def kernel(
    dims, den_hbm, pot_hbm, rw_hbm, cw_hbm, out_ref,
    den_v, pot_v, rw, cw, cp, cpy, cd, cdy, cf, cl,
    z1s, z1r, z1y, zfs, zfr, zls, zlr,
    R, B, SR, SB, LR, LB, ER, EB, gat, cv, dummy,
    ssem, rsem, lsem,
):
    nx, ny, nz, X, Y, Z = dims
    n = nx * ny * nz
    I, J, K = X // 2, Y // 2, Z // 2
    T, T1 = J + 2 * H, J + 2 * H1
    M = I // 2
    ring = nx == 2 and I < DEEP
    E = 0 if ring else 5
    G, F, GL = X // 4, max(X // 12, 1), M // 3
    FW = X // F
    assert X % 12 == 0 and FW <= 12 and 2 * K <= 128 and J % 8 == 0 and 2 * J > DEEP and 2 * M >= E and M % 3 == 0
    names = offsets(nx, ny, nz)
    NF = len(names)
    Q = -(-(NF + 1) // 8) * 8
    ix, iy, iz = lax.axis_index("gx"), lax.axis_index("gy"), lax.axis_index("gz")
    me = (ix * ny + iy) * nz + iz

    def around(i, count):
        return [i] + [jnp.where(i + o >= count, i + o - count, i + o) for o in range(1, count)]

    xs, ys, zs = around(ix, nx), around(iy, ny), around(iz, nz)

    def device(o):
        if isinstance(o, int):
            return (xs[o // (ny * nz)], ys[o // nz % ny], zs[o % nz])
        ox, oy, oz = o // (ny * nz), (o // nz) % ny, o % nz
        return (lax.rem(ix + ox, nx), lax.rem(iy + oy, ny), lax.rem(iz + oz, nz))

    def each_other(step):
        if n <= 64:
            for o in range(1, n):
                step(o, 0)
        else:
            lax.fori_loop(1, n, step, 0)

    wide = (lambda ref: ref) if Z == 128 else (lambda ref: ref.at[:, :, pl.ds(0, Z)])
    load_p = pltpu.make_async_copy(pot_hbm, wide(pot_v), lsem.at[0])
    load_d = pltpu.make_async_copy(den_hbm, wide(den_v), lsem.at[1])
    load_rw = pltpu.make_async_copy(rw_hbm, rw, lsem.at[2])
    load_cw = pltpu.make_async_copy(cw_hbm, cw, lsem.at[3])

    barrier = pltpu.get_barrier_semaphore()

    def greet(o, carry):
        pl.semaphore_signal(barrier, inc=1, device_id=device(o), device_id_type=MESH)
        return carry

    near = max(nx, ny, nz) <= 5
    steps = sorted({
        (dx % nx * ny + dy % ny) * nz + dz % nz
        for dx in (-1, 0, 1) for dy in (-1, 0, 1) for dz in (-1, 0, 1)
    } - {0})
    if near:
        for o in sorted(steps, key=lambda o: o // nz % ny == 0):
            greet(o, 0)
    else:
        each_other(greet)
    load_p.start()
    load_d.start()
    load_rw.start()
    load_cw.start()

    up = {1: iy > 0, -1: iy == 0}

    def along_y(d):
        if d == 0:
            return iy
        return jnp.where(up[1 if d > 0 else -1], ys[abs(d)], ys[-abs(d)])

    target_y = {d: along_y(d) for d in (0, 1, -1) + ((2, -2) if ny > 2 else ())}

    def part_y(d, own, count, first, low=None, high=None):
        if d == 0:
            return first, own, first
        low = first - count if low is None else low
        high = first + own if high is None else high
        goes_up = up[1 if d > 0 else -1]
        return jnp.where(goes_up, first + own - count, first), count, jnp.where(goes_up, low, high)

    class Exchange:
        def __init__(self, k):
            self.k, self.rows = k, 0

        def send(self, src, dst, at, to):
            dx, dy, dz = to
            copy = pltpu.make_async_remote_copy(
                src_ref=src, dst_ref=dst, send_sem=ssem.at[self.k], recv_sem=rsem.at[self.k],
                device_id=(xs[dx], target_y[dy], zs[dz]), device_id_type=MESH,
            )
            copy.start()
            self.rows += at

        def wait(self):
            all_of = dummy.at[pl.ds(0, self.rows)]
            pltpu.make_async_copy(all_of, all_of, rsem.at[self.k]).wait()
            pltpu.make_async_copy(all_of, all_of, ssem.at[self.k]).wait()

    def part(d, own, count, first):
        if d == 0:
            return first, own, first
        if d == 1:
            return first + own - count, count, first - count
        return first, count, first + own

    def block(ex, src, dst, px, py, to, shift=0, lead=None):
        (sx, cx, tx), (sy, cy, ty) = px, py
        target = dst if lead is None else dst.at[lead]
        ex.send(
            src.at[pl.ds(sx, cx), pl.ds(sy - shift, cy)],
            target.at[pl.ds(tx, cx), pl.ds(ty, cy)],
            cx * cy, to,
        )

    def iota(rows, dim):
        return lax.broadcasted_iota(jnp.int32, (rows, 128), dim)

    lane = {rows: iota(rows, 1) for rows in {8, J, T, T1}}

    def place(acc, v, pieces):
        by_shift = {}
        for src, dst, width in pieces:
            by_shift.setdefault((dst - src) % 128, []).append((dst, width))
        at = lane[v.shape[0]]
        for shift, spans in by_shift.items():
            mask = None
            for dst, width in spans:
                inside = (at >= dst) & (at < dst + width)
                mask = inside if mask is None else mask | inside
            moved = turn(v, shift)
            acc = jnp.where(mask, moved, acc)
        return acc

    def outside(z, right, left):
        if (right - left) % 128 == 0:
            return turn(z, right)
        return jnp.where(lane[z.shape[0]] < 96, turn(z, right), turn(z, left))

    def with_sides(v, half, z, right, left):
        own = turn(v, -K) if half else v
        if z is None:
            return own
        return jnp.where(lane[v.shape[0]] < K, own, outside(z, right, left))

    def two(a, b):
        return jnp.where(lane[a.shape[0]] < K, a, turn(b, K))

    l8 = lane[J]
    low = jnp.where(l8 < K, 2 * l8, 2 * (l8 - K) + 1) & 127
    high = jnp.where(l8 < K, 2 * l8 + 1, 2 * (l8 - K)) & 127
    order = (low, high)

    def colours(ref, x, which):
        v = [ref[x, pl.ds(b, J, stride=2), :] for b in (0, 1)]
        take = [jnp.take_along_axis(u, order[which], axis=1, mode="promise_in_bounds") for u in v]
        return jnp.where(l8 < K, take[0], take[1])

    def plane(x, deep):
        if 0 <= x < X:
            return (x + X // 2) % X
        return X + deep + x if x < 0 else deep + x

    def tile(x, t):
        if 0 <= x < X:
            return 2 * plane(x, 4) + (t if x < X // 2 else 1 - t)
        return 2 * X + (6 + 2 * (x + 1) - t if x < 0 else 7 + 2 * (x - X) + t)

    def group(g):
        return 0 if g < 0 else (1 if g >= G else 2 + (g + 1) % G)

    def along_x(count, middle, halo, halo_size):
        if nx == 2:
            return [(1, (middle - count, 2 * count, halo + halo_size - count))]
        return [(1, (middle - count, count, halo + halo_size - count)), (-1, (middle, count, halo + halo_size))]

    def groups_x():
        return [(1, (0, 2, 0))] if nx == 2 else [(1, (0, 1, 0)), (-1, (1, 1, 1))]

    load_p.wait()
    load_d.wait()
    total = jnp.zeros((J, 128), jnp.float32)
    for g in range(G):
        acc = jnp.zeros((J, 128), jnp.float32)
        for q in range(4):
            x = 4 * g + q
            black = colours(pot_v, x, 1 - x % 2)
            dens = [colours(den_v, x, x % 2), colours(den_v, x, 1 - x % 2)]
            cp[plane(x, 5)] = black
            acc = place(acc, black, [
                p for h in (0, 1)
                for p in ((h * K, 15 * q + 3 * h, 3), (h * K + K - 3, 61 + 15 * q + 3 * h, 3))
            ])
            for t in (0, 1):
                cd[tile(x, t)] = dens[t]
                total = total + dens[t]
                acc = place(acc, dens[t], [
                    p for h in (0, 1) for o in (15 * q + 6 + 4 * t + 2 * h,)
                    for p in ((h * K, o, 2), (h * K + K - 2, 62 + o, 2))
                ])
        z1s[(g + 1) % G] = acc
    total = jnp.where(l8 < 2 * K, total, 0.0)

    pl.semaphore_wait(barrier, len(steps) if near else n - 1)
    first, first_y = Exchange(0), Exchange(3)

    def rim(dy, rows, skip=0):
        return part_y(dy, J - skip, rows, 0, 8 - skip - rows, skip) if not skip else (
            jnp.where(up[dy], J - skip - rows, skip), rows, jnp.where(up[dy], 8 - skip - rows, skip))

    for dy in (A, B_):
        for count, skip in ((4, 0), (2, 1)):
            for dx, px in along_x(count, X // 2, X, 5):
                block(first_y, cp, cpy, px, rim(dy, 1, skip), (dx, dy, 0))
        for count, skip in ((5, 0), (2, 1)):
            for dx, px in along_x(count, X, 2 * X, 7):
                block(first_y, cd, cdy, px, rim(dy, 1, skip), (dx, dy, 0))
        for dx, px in groups_x():
            for dz in (1, -1):
                block(first_y, z1s, z1y, px, rim(dy, 2), (dx, dy, dz), 0, max(dz, 0))
        block(first_y, cp, cpy, (0, X, 0), rim(dy, 3), (0, dy, 0))
        block(first_y, cd, cdy, (0, 2 * X, 0), rim(dy, 2), (0, dy, 0))
        for dz in (1, -1):
            block(first_y, z1s, z1y, (0, G, 2), rim(dy, 2), (0, dy, dz), 0, max(dz, 0))
    whole_rows = (0, J, 0)
    for dz in (1, -1):
        block(first, z1s, z1r, (0, G, 2), whole_rows, (0, 0, dz), 0, max(dz, 0))
        for dx, px in groups_x():
            block(first, z1s, z1r, px, whole_rows, (dx, 0, dz), 0, max(dz, 0))
    for dx, px in along_x(5, X // 2, X, 5):
        block(first, cp, cp, px, whole_rows, (dx, 0, 0))
    for dx, px in along_x(7, X, 2 * X, 7):
        block(first, cd, cd, px, whole_rows, (dx, 0, 0))

    def base(x, b):
        return 8 + ((x + 5) * 2 + b) * T

    def get(ref, x, b, off=0):
        return ref[pl.ds(base(x, b) + off, T), :]

    def own(ref, x, b, off=0):
        return ref[pl.ds(base(x, b) + H + off, J), :]

    sides = {}

    def side(x, ref, rows):
        key = (x // 4, rows)
        if key not in sides:
            sides[key] = jnp.where(lane[rows] < 60, ref[0, group(key[0])], ref[1, group(key[0])])
        return sides[key]

    def unpack(tiles, dens, zs_, rows, less, put):
        for x in range(-5, X + 5):
            far = max(-x, x - X + 1, 0) + less
            z = side(x, zs_, rows) if far < 5 else None
            if far <= 5:
                for h in (0, 1):
                    s = 15 * (x % 4) + 3 * h
                    put(B, x, h, with_sides(tiles[plane(x, 5)], h, z, K - s, 64 - s))
            for t, ref in ((0, SR), (1, SB)):
                z = side(x, zs_, rows) if far < 4 - t else None
                if far <= 4 - t:
                    for h in (0, 1):
                        s = 15 * (x % 4) + 6 + 4 * t + 2 * h
                        put(ref, x, h, with_sides(dens[tile(x, t)], h, z, K - s, 64 - s))

    def put_middle(ref, x, h, v):
        ref[pl.ds(base(x, h) + H, J), :] = v

    def put_rim(ref, x, h, v):
        ref[pl.ds(base(x, h) + H - 3, 3), :] = v[5:8]
        ref[pl.ds(base(x, h) + H + J, 3), :] = v[0:3]

    load_rw.wait()
    load_cw.wait()
    first.wait()
    unpack(cp, cd, z1r, J, 0, put_middle)
    first_y.wait()
    sides.clear()
    unpack(cpy, cdy, z1y, 8, 1, put_rim)
    sides.clear()

    sixth = jnp.float32(1.0 / 6.0)

    def beside(read, v, x, b, colour):
        c = (x + b + colour) % 2
        mid = read(v, x, b)
        t = read(v, x - 1, b) + read(v, x + 1, b)
        t = t + (read(v, x, 1 - b) + read(v, x, 1 - b, 2 * b - 1))
        return t + (mid + turn(mid, 1 - 2 * c))

    def half(depth, colour):
        new, old, src = ((R, B, SR), (B, R, SB))[colour]
        for x in range(-depth, X + depth):
            for b in (0, 1):
                new[pl.ds(base(x, b), T), :] = (beside(get, old, x, b, colour) - get(src, x, b)) * sixth

    for k in range(4):
        half(4 - k, k % 2)

    def even_at(rows):
        return (iota(rows, 0) + lane[rows]) % 2 == 0

    even = {rows: even_at(rows) for rows in {J, T}}
    one = []
    for i in range(I):
        left = None
        for x in (2 * i, 2 * i + 1):
            for b in (0, 1):
                for colour, (v, w, s) in enumerate(((R, B, SR), (B, R, SB))):
                    r = own(s, x, b) - (beside(own, w, x, b, colour) - 6.0 * own(v, x, b))
                    left = r if left is None else left + r
        one.append(left * 0.5)
    sums = [jnp.zeros((J, 128), jnp.float32) for _ in names]
    for g in range(GL):
        acc = jnp.zeros((J, 128), jnp.float32)
        for q in range(3):
            m = 3 * g + q
            red = jnp.where(even[J], one[2 * m], one[2 * m + 1])
            black = jnp.where(even[J], one[2 * m + 1], one[2 * m])
            both = two(red, black)
            if 2 * K < 128:
                both = jnp.where(l8 < 2 * K, both, 0.0)
            cl[E + m, H1 : H1 + J] = both
            sums = [a + rw[f, m] * both for f, a in enumerate(sums)]
            for c, v in enumerate((red, black)):
                s = 18 * q + 9 * c
                acc = place(acc, v, [(0, s, DEEP), (K - DEEP, 55 + s, DEEP)])
        zls[g] = acc

    def stack(rows):
        rows = [jnp.sum(v, axis=0, keepdims=True) for v in rows]
        rows = rows + [jnp.zeros((1, 128), jnp.float32)] * (Q - len(rows))
        return jnp.sum(jnp.concatenate(rows, axis=0), axis=1, keepdims=True)

    spot = lax.broadcasted_iota(jnp.int32, (Q, 128), 0) == lax.broadcasted_iota(jnp.int32, (Q, 128), 1)
    gat[0] = jnp.sum(jnp.where(spot, stack(sums + [total]), 0.0), axis=0, keepdims=True)

    def spread(o, carry):
        if isinstance(o, int):
            there = ((-(o // (ny * nz)) % nx) * ny + -(o // nz) % ny) * nz + -o % nz
        else:
            ox, oy, oz = o // (ny * nz), (o // nz) % ny, o % nz
            there = (lax.rem(nx - ox, nx) * ny + lax.rem(ny - oy, ny)) * nz + lax.rem(nz - oz, nz)
        pltpu.make_async_remote_copy(
            src_ref=gat.at[0], dst_ref=gat.at[there], send_sem=ssem.at[2], recv_sem=rsem.at[2],
            device_id=device(o), device_id_type=MESH,
        ).start()
        return carry

    def spread_y(d):
        for dx in range(nx):
            for dz in range(nz):
                if d == 0 and dx == 0 and dz == 0:
                    continue
                slot = [(-dx % nx * ny + dy % ny) * nz + -dz % nz for dy in (-abs(d), abs(d))]
                there = jnp.where(up[d], slot[0], slot[1]) if abs(d) == 1 else slot[0]
                where_y = target_y[d] if abs(d) == 1 else ys[d]
                pltpu.make_async_remote_copy(
                    src_ref=gat.at[0], dst_ref=gat.at[there], send_sem=ssem.at[2], recv_sem=rsem.at[2],
                    device_id=(xs[dx], where_y, zs[dz]), device_id_type=MESH,
                ).start()

    by_rows = n <= 64 and ny > 2
    if by_rows:
        spread_y(A)
    else:
        each_other(spread)

    second = Exchange(1)

    def deep(d, own, count, first):
        if abs(d) < 2:
            return part(d, own, min(own, count), first)
        count -= own
        return (first + own - count, count, first - own - count) if d > 0 else (first, count, first + 2 * own)

    def deep_y(d, own, count, first):
        if abs(d) < 2:
            return part_y(d, own, min(own, count), first)
        count -= own
        return part_y(d, own, count, first, first - own - count, first + 2 * own)

    def send_deep(dy):
        for dx in (1, 0) if ring else (1, -1, 0, 2, -2):
            if abs(dx) + abs(dy) > 3 or (abs(dy) == 2 and J >= DEEP) or (abs(dx) == 2 and M >= E):
                continue
            px = (0, M, M if dx else 0) if ring else deep(dx, M, E, E)
            pz = (0, GL, GL * dx) if ring else (0, GL, GL * (2 - dx))
            py = deep_y(dy, J, DEEP, H1)
            for dz in (1, -1):
                block(second, zls, zlr, pz, py, (dx, dy, dz), H1, max(dz, 0))
            if dx or dy:
                block(second, cl, cl, px, py, (dx, dy, 0))

    send_deep(A)
    if by_rows:
        for d in range(2, ny - 1):
            spread_y(d)
        spread_y(B_)
    send_deep(AA)
    send_deep(BB)
    send_deep(B_)
    send_deep(0)
    if by_rows:
        spread_y(0)

    for f in range(F):
        acc = jnp.zeros((J, 128), jnp.float32)
        for q in range(FW):
            x = f * FW + q
            v = two(own(B, x, 0), own(B, x, 1))
            cf[plane(x, 4), H : H + J] = v
            acc = place(acc, v, [
                p for h in (0, 1) for o in (4 * q + 2 * h,)
                for p in ((h * K, o, 2), (h * K + K - 2, 62 + o, 2))
            ])
        zfs[f] = acc
    fourth = Exchange(4)
    twice = nx == 2 and F == 1
    for dy in (A, B_, 0):
        for dx, px in along_x(3 if dy else 4, X // 2, X, 4):
            block(fourth, cf, cf, px, part_y(dy, J, 2, H), (dx, dy, 0))
        if dy:
            block(fourth, cf, cf, (0, X, 0), part_y(dy, J, 2, H), (0, dy, 0))
        for dx in (1, 0) if twice else (1, -1, 0):
            for dz in (1, -1):
                g0, gn, g1 = part(dx, F, 1, 1)
                block(fourth, zfs, zfr, (g0 - 1, gn, g1), part_y(dy, J, 2, H), (dx, dy, dz), H, max(dz, 0))

    others = gat.at[pl.ds(0, n - 1)]
    pltpu.make_async_copy(others, others, rsem.at[2]).wait()
    pltpu.make_async_copy(others, others, ssem.at[2]).wait()
    values = gat[:, 0, :]
    whole = jnp.sum(values, axis=0, keepdims=True)
    values = values - whole / jnp.float32(n)
    lane1 = lax.broadcasted_iota(jnp.int32, (1, 128), 1)
    cv[...] = jnp.broadcast_to(
        stack([cw[o] * values for o in range(NF)] + [jnp.where(lane1 == NF, whole, 0.0)]), (Q, 128)
    )
    mean = cv[NF : NF + 1, :] / jnp.float32(n * X * Y * Z)
    row = iota(T1, 0)
    at = lane[T1]
    maps = {}
    for dx in ((0, 1) if ring else (0, 1, -1)):
        by_row = []
        for dy in (-1, 0, 1):
            vals = [cv[names.index((dx % nx, dy % ny, dz % nz)), :][None] for dz in (-1, 0, 1)]
            by_row.append(jnp.where(at < K, vals[1], jnp.where(at < (K + 128) // 2, vals[2], vals[0])))
        field = jnp.where(row < H1, by_row[0], jnp.where(row < H1 + J, by_row[1], by_row[2]))
        maps[dx] = field + mean * jnp.float32(8.0 / 3.0)

    def base1(m):
        return 8 + ((m % (2 * M)) if ring else m + 6) * T1

    def span(depth):
        low, high = (-depth) // 2, (I - 1 + depth) // 2
        return range(2 * M) if ring and high - low + 1 >= 2 * M else range(low, high + 1)

    def window(depth):
        reach = -(-depth // 4) * 4
        return H1 - reach, J + 2 * reach

    def get1(ref, m, start, rows):
        return ref[pl.ds(base1(m) + start, rows), :]

    second.wait()
    sides.clear()
    for m in span(DEEP):
        g, q = m // 3 + (0 if ring else 2 * GL), m % 3
        if g not in sides:
            sides[g] = jnp.where(lane[T1] < 55, zlr[0, g], zlr[1, g])
        for c, ref in ((0, LR), (1, LB)):
            s = 18 * q + 9 * c
            ref[pl.ds(base1(m), T1), :] = with_sides(cl[m + E], c, sides[g], K - s, 64 - s)

    masks = {}

    def even_from(start, rows):
        if rows not in masks:
            masks[rows] = (lax.broadcasted_iota(jnp.int32, (rows, 128), 0) + lax.broadcasted_iota(jnp.int32, (rows, 128), 1)) % 2 == 0
        return masks[rows] if start % 2 == 0 else jnp.logical_not(masks[rows])

    def half1(depth, colour, shift=None, start_red=False):
        new, old, src = ((ER, EB, LR), (EB, ER, LB))[colour]
        if start_red:
            old = LR
        start, rows = window(depth)
        mask = even_from(start, rows)
        for m in span(depth):
            c = get1(old, m, start, rows)
            before, after = get1(old, m - 1, start, rows), get1(old, m + 1, start, rows)
            t = c + (jnp.where(mask, before, after) if colour == 0 else jnp.where(mask, after, before))
            t = t + (get1(old, m, start - 1, rows) + get1(old, m, start + 1, rows))
            t = t + (turn(c, 1) + turn(c, -1))
            t = (t * -sixth if start_red else t) - get1(src, m, start, rows)
            if shift is not None:
                t = t + shift
            new[pl.ds(base1(m) + start, rows), :] = t * sixth

    half1(8, 1, start_red=True)
    half1(7, 0)
    half1(6, 1)
    for m in span(6):
        dx = (0 if 0 <= m < M else 1) if ring else (-1 if m < 0 else (0 if m < M else 1))
        start, rows = window(6)
        EB[pl.ds(base1(m) + start, rows), :] = get1(EB, m, start, rows) + maps[dx][start : start + rows]
    shift = 4.0 * mean
    half1(5, 0, shift)
    half1(4, 1, shift)
    half1(3, 0, shift)
    half1(2, 1, shift)

    fourth.wait()
    sides.clear()
    rise = mean * jnp.float32(2.0 / 3.0)
    for m in range(-1, M + 1):
        tiles = [get1(v, m, H1 - H, T) for v in (ER, EB)]
        for i in (2 * m, 2 * m + 1):
            first_, second_ = tiles if i % 2 == 0 else tiles[::-1]
            e = jnp.where(even[T], first_, second_) + rise
            for x in (2 * i, 2 * i + 1):
                far = max(-x, x - X + 1, 0)
                z = None
                if far < 4:
                    f = 0 if x < 0 or (x >= X and twice) else (F + 1 if x >= X else x // FW + 1)
                    if f not in sides:
                        sides[f] = jnp.where(lane[T] < 60, zfr[0, f], zfr[1, f])
                    z = sides[f]
                for h in (0, 1):
                    s = 4 * (x % FW) + 2 * h
                    B[pl.ds(base(x, h), T), :] = with_sides(cf[plane(x, 4)], h, z, K - s, 64 - s) + e

    def last(depth, colour):
        new, old, src = ((R, B, SR), (B, R, SB))[colour]
        for x in range(-depth, X + depth):
            for b in (0, 1):
                t = beside(get, old, x, b, colour) - get(src, x, b) + mean
                new[pl.ds(base(x, b), T), :] = t * sixth

    last(3, 0)
    last(2, 1)
    last(1, 0)
    back = l8 >> 1
    odd_lane = (l8 & 1) == 1
    for x in range(X):
        for b in (0, 1):
            red = own(R, x, b)
            dark = (beside(own, R, x, b, 1) - own(SB, x, b) + mean) * sixth
            pair = (red, dark) if (x + b) % 2 == 0 else (dark, red)
            e, o = (jnp.take_along_axis(v, back, axis=1, mode="promise_in_bounds") for v in pair)
            out_ref[x, pl.ds(b, J, stride=2), :] = jnp.where(odd_lane, o, e)[:, 0:Z]


def body(dims, density, potential):
    nx, ny, nz, X, Y, Z = dims
    n = nx * ny * nz
    I, J, K = X // 2, Y // 2, Z // 2
    T, T1 = J + 2 * H, J + 2 * H1
    M = I // 2
    ring = nx == 2 and I < DEEP
    G, F, GL = X // 4, max(X // 12, 1), M // 3
    op = coarse_operator(nx, ny, nz, float(J * K), float(I * K), float(I * J))
    rw = residual_weights(nx, ny, nz, I, J, K)
    cw = coarse_weights(op, nx, ny, nz)
    Q = -(-(len(rw) + 1) // 8) * 8
    fine = 16 + (X + 10) * 2 * T
    coarse = 16 + (2 * M if ring else M + 12) * T1

    def vmem(*shape):
        return pltpu.VMEM(shape, jnp.float32)

    return pl.pallas_call(
        functools.partial(kernel, dims),
        out_shape=pltpu.VMEM((X, Y, Z), jnp.float32),
        in_specs=[pl.BlockSpec(memory_space=pl.ANY)] * 4,
        out_specs=pl.BlockSpec(memory_space=pltpu.VMEM),
        scratch_shapes=[
            vmem(X, Y, 128),
            vmem(X, Y, 128),
            vmem(*rw.shape),
            vmem(*cw.shape),
            vmem(X + 10, J, 128),
            vmem(X + 10, 8, 128),
            vmem(2 * X + 14, J, 128),
            vmem(2 * X + 14, 8, 128),
            vmem(X + 8, T, 128),
            vmem(2 * M if ring else M + 10, T1, 128),
            vmem(G, J, 128),
            vmem(2, G + 2, J, 128),
            vmem(2, G + 2, 8, 128),
            vmem(F, J, 128),
            vmem(2, F + 2, T, 128),
            vmem(GL, J, 128),
            vmem(2, (2 if ring else 5) * GL, T1, 128),
            vmem(fine, 128),
            vmem(fine, 128),
            vmem(fine, 128),
            vmem(fine, 128),
            vmem(coarse, 128),
            vmem(coarse, 128),
            vmem(coarse, 128),
            vmem(coarse, 128),
            vmem(n, 1, 128),
            vmem(Q, 128),
            vmem(2048, 128),
            pltpu.SemaphoreType.DMA((5,)),
            pltpu.SemaphoreType.DMA((5,)),
            pltpu.SemaphoreType.DMA((4,)),
        ],
        compiler_params=pltpu.CompilerParams(collective_id=0, has_side_effects=True),
        name="vcycle",
    )(density, potential, rw, cw)


def solution(mesh):
    nx, ny, nz = (mesh.shape[a] for a in ("gx", "gy", "gz"))

    def run(density, potential):
        return body((nx, ny, nz) + density.shape, density, potential)

    spec = P("gx", "gy", "gz")
    return jax.shard_map(run, mesh=mesh, in_specs=(spec, spec), out_specs=spec, check_vma=False)
```

```python
import functools
import numpy as np
import jax
import jax.numpy as jnp
from jax import lax
from jax.experimental import pallas as pl
from jax.experimental.pallas import tpu as pltpu
from jax.sharding import PartitionSpec as P

HI = lax.Precision.HIGHEST
MESH = pl.DeviceIdType.MESH
H, H1 = 4, 12
DEEP = 9
A, B_, AA, BB = 1, -1, 2, -2
SIDES = ((1, A), (-1, A), (0, A), (1, B_), (-1, B_), (0, B_), (0, 0), (1, 0), (-1, 0))


def table(count):
    modes = (np.arange(count) + 1) // 2
    angle = 2 * np.pi * np.outer(np.arange(count), modes) / count
    q = np.where(np.arange(count) % 2 == 1, np.cos(angle), np.sin(angle)) * np.sqrt(2 / count)
    q = np.where(2 * modes == count, np.cos(angle) / np.sqrt(count), q)
    q[:, 0] = 1 / np.sqrt(count)
    return q, 2 - 2 * np.cos(2 * np.pi * modes / count)


def coarse_operator(nx, ny, nz, wx, wy, wz):
    qx, lx = table(nx)
    qy, ly = table(ny)
    qz, lz = table(nz)
    q = np.kron(np.kron(qx, qy), qz)
    lam = wx * lx[:, None, None] + wy * ly[None, :, None] + wz * lz[None, None, :]
    lam = lam.reshape(-1)
    inv = np.concatenate([[0.0], -1.0 / lam[1:]])
    return ((q * inv) @ q.T).astype(np.float32)


def offsets(nx, ny, nz):
    steps = [(dx % nx, dy % ny, dz % nz) for dx in (0, 1, -1) for dy in (0, 1, -1) for dz in (0, 1, -1)]
    return list(dict.fromkeys(steps))


def residual_weights(nx, ny, nz, I, J, K):
    block = np.zeros((3 * I, 3 * J, 3 * K))
    block[I : 2 * I, J : 2 * J, K : 2 * K] = 1.0

    def beside(v):
        return sum(np.roll(v, d, axis) for axis in range(3) for d in (1, -1))

    red = np.indices(block.shape).sum(0) % 2 == 0
    v = beside(block) - 6.0 * block
    black2 = np.where(red, 0.0, v)
    red2 = np.where(red, v + beside(black2) / 6.0, 0.0)
    black1 = np.where(red, 0.0, beside(red2) / 6.0)
    red1 = np.where(red, beside(black1) / 6.0, 0.0)
    w = block + (black2 + red2 + black1 + red1) / 6.0
    names = offsets(nx, ny, nz)
    own = np.zeros((len(names), I, J, K))
    for dx in (0, 1, -1):
        for dy in (0, 1, -1):
            for dz in (0, 1, -1):
                x, y, z = (1 - dx) * I, (1 - dy) * J, (1 - dz) * K
                own[names.index((dx % nx, dy % ny, dz % nz))] += w[x : x + I, y : y + J, z : z + K]
    even = np.indices((J, K)).sum(0) % 2 == 0
    first, second = own[:, 0::2], own[:, 1::2]
    out = np.zeros((len(names), I // 2, J, 128))
    out[..., :K] = np.where(even, first, second)
    out[..., K : 2 * K] = np.where(even, second, first)
    return out.astype(np.float32)


def coarse_weights(op, nx, ny, nz):
    names = offsets(nx, ny, nz)
    green = op.astype(np.float64)[:, 0].reshape(nx, ny, nz)
    rx, ry, rz = np.indices((nx, ny, nz)).reshape(3, -1)
    out = np.zeros((len(names), nx * ny * nz, 128))
    for o, (ox, oy, oz) in enumerate(names):
        for f, (fx, fy, fz) in enumerate(names):
            out[o, :, f] = green[(ox - rx - fx) % nx, (oy - ry - fy) % ny, (oz - rz - fz) % nz]
    return out.astype(np.float32)


def turn(v, shift):
    shift %= 128
    return pltpu.roll(v, shift, 1) if shift else v


def kernel(
    dims, den_hbm, pot_hbm, rw_hbm, cw_hbm, out_ref,
    den_v, pot_v, rw, cw, cp, cpy, cd, cdy, cf, cl,
    z1s, z1r, z1y, zfs, zfr, zls, zlr,
    R, B, SR, SB, LR, LB, ER, EB, gat, cv, dummy,
    ssem, rsem, lsem,
):
    nx, ny, nz, X, Y, Z = dims
    n = nx * ny * nz
    I, J, K = X // 2, Y // 2, Z // 2
    T, T1 = J + 2 * H, J + 2 * H1
    M = I // 2
    ring = nx == 2 and I < DEEP
    E = 0 if ring else 5
    G, F, GL = X // 4, max(X // 12, 1), M // 3
    FW = X // F
    assert X % 12 == 0 and FW <= 12 and 2 * K <= 128 and J % 8 == 0 and 2 * J > DEEP and 2 * M >= E and M % 3 == 0
    names = offsets(nx, ny, nz)
    NF = len(names)
    Q = -(-(NF + 1) // 8) * 8
    ix, iy, iz = lax.axis_index("gx"), lax.axis_index("gy"), lax.axis_index("gz")
    me = (ix * ny + iy) * nz + iz

    def around(i, count):
        return [i] + [jnp.where(i + o >= count, i + o - count, i + o) for o in range(1, count)]

    xs, ys, zs = around(ix, nx), around(iy, ny), around(iz, nz)

    def device(o):
        if isinstance(o, int):
            return (xs[o // (ny * nz)], ys[o // nz % ny], zs[o % nz])
        ox, oy, oz = o // (ny * nz), (o // nz) % ny, o % nz
        return (lax.rem(ix + ox, nx), lax.rem(iy + oy, ny), lax.rem(iz + oz, nz))

    def each_other(step):
        if n <= 64:
            for o in range(1, n):
                step(o, 0)
        else:
            lax.fori_loop(1, n, step, 0)

    wide = (lambda ref: ref) if Z == 128 else (lambda ref: ref.at[:, :, pl.ds(0, Z)])
    load_p = pltpu.make_async_copy(pot_hbm, wide(pot_v), lsem.at[0])
    load_d = pltpu.make_async_copy(den_hbm, wide(den_v), lsem.at[1])
    load_rw = pltpu.make_async_copy(rw_hbm, rw, lsem.at[2])
    load_cw = pltpu.make_async_copy(cw_hbm, cw, lsem.at[3])

    barrier = pltpu.get_barrier_semaphore()

    def greet(o, carry):
        pl.semaphore_signal(barrier, inc=1, device_id=device(o), device_id_type=MESH)
        return carry

    near = max(nx, ny, nz) <= 5
    steps = sorted({
        (dx % nx * ny + dy % ny) * nz + dz % nz
        for dx in (-1, 0, 1) for dy in (-1, 0, 1) for dz in (-1, 0, 1)
    } - {0})
    if near:
        for o in sorted(steps, key=lambda o: o // nz % ny == 0):
            greet(o, 0)
    else:
        each_other(greet)
    load_p.start()
    load_d.start()
    load_rw.start()
    load_cw.start()

    up = {1: 2 * iy >= ny, -1: 2 * iy < ny}

    def along_y(d):
        if d == 0:
            return iy
        return jnp.where(up[1 if d > 0 else -1], ys[abs(d)], ys[-abs(d)])

    target_y = {d: along_y(d) for d in (0, 1, -1) + ((2, -2) if ny > 2 else ())}

    def part_y(d, own, count, first, low=None, high=None):
        if d == 0:
            return first, own, first
        low = first - count if low is None else low
        high = first + own if high is None else high
        goes_up = up[1 if d > 0 else -1]
        return jnp.where(goes_up, first + own - count, first), count, jnp.where(goes_up, low, high)

    class Exchange:
        def __init__(self, k):
            self.k, self.rows = k, 0

        def send(self, src, dst, at, to):
            dx, dy, dz = to
            copy = pltpu.make_async_remote_copy(
                src_ref=src, dst_ref=dst, send_sem=ssem.at[self.k], recv_sem=rsem.at[self.k],
                device_id=(xs[dx], target_y[dy], zs[dz]), device_id_type=MESH,
            )
            copy.start()
            self.rows += at

        def wait(self):
            all_of = dummy.at[pl.ds(0, self.rows)]
            pltpu.make_async_copy(all_of, all_of, rsem.at[self.k]).wait()
            pltpu.make_async_copy(all_of, all_of, ssem.at[self.k]).wait()

    def part(d, own, count, first):
        if d == 0:
            return first, own, first
        if d == 1:
            return first + own - count, count, first - count
        return first, count, first + own

    def block(ex, src, dst, px, py, to, shift=0, lead=None):
        (sx, cx, tx), (sy, cy, ty) = px, py
        target = dst if lead is None else dst.at[lead]
        ex.send(
            src.at[pl.ds(sx, cx), pl.ds(sy - shift, cy)],
            target.at[pl.ds(tx, cx), pl.ds(ty, cy)],
            cx * cy, to,
        )

    def iota(rows, dim):
        return lax.broadcasted_iota(jnp.int32, (rows, 128), dim)

    lane = {rows: iota(rows, 1) for rows in {8, J, T, T1}}

    def place(acc, v, pieces):
        by_shift = {}
        for src, dst, width in pieces:
            by_shift.setdefault((dst - src) % 128, []).append((dst, width))
        at = lane[v.shape[0]]
        for shift, spans in by_shift.items():
            mask = None
            for dst, width in spans:
                inside = (at >= dst) & (at < dst + width)
                mask = inside if mask is None else mask | inside
            moved = turn(v, shift)
            acc = jnp.where(mask, moved, acc)
        return acc

    def outside(z, right, left):
        if (right - left) % 128 == 0:
            return turn(z, right)
        return jnp.where(lane[z.shape[0]] < 96, turn(z, right), turn(z, left))

    def with_sides(v, half, z, right, left):
        own = turn(v, -K) if half else v
        if z is None:
            return own
        return jnp.where(lane[v.shape[0]] < K, own, outside(z, right, left))

    def two(a, b):
        return jnp.where(lane[a.shape[0]] < K, a, turn(b, K))

    l8 = lane[J]
    low = jnp.where(l8 < K, 2 * l8, 2 * (l8 - K) + 1) & 127
    high = jnp.where(l8 < K, 2 * l8 + 1, 2 * (l8 - K)) & 127
    order = (low, high)

    def colours(ref, x, which):
        v = [ref[x, pl.ds(b, J, stride=2), :] for b in (0, 1)]
        take = [jnp.take_along_axis(u, order[which], axis=1, mode="promise_in_bounds") for u in v]
        return jnp.where(l8 < K, take[0], take[1])

    def plane(x, deep):
        if 0 <= x < X:
            return (x + X // 2) % X
        return X + deep + x if x < 0 else deep + x

    def tile(x, t):
        if 0 <= x < X:
            return 2 * plane(x, 4) + (t if x < X // 2 else 1 - t)
        return 2 * X + (6 + 2 * (x + 1) - t if x < 0 else 7 + 2 * (x - X) + t)

    def group(g):
        return 0 if g < 0 else (1 if g >= G else 2 + (g + 1) % G)

    def along_x(count, middle, halo, halo_size):
        if nx == 2:
            return [(1, (middle - count, 2 * count, halo + halo_size - count))]
        return [(1, (middle - count, count, halo + halo_size - count)), (-1, (middle, count, halo + halo_size))]

    def groups_x():
        return [(1, (0, 2, 0))] if nx == 2 else [(1, (0, 1, 0)), (-1, (1, 1, 1))]

    load_p.wait()
    load_d.wait()
    total = jnp.zeros((J, 128), jnp.float32)
    for g in range(G):
        acc = jnp.zeros((J, 128), jnp.float32)
        for q in range(4):
            x = 4 * g + q
            black = colours(pot_v, x, 1 - x % 2)
            dens = [colours(den_v, x, x % 2), colours(den_v, x, 1 - x % 2)]
            cp[plane(x, 5)] = black
            acc = place(acc, black, [
                p for h in (0, 1)
                for p in ((h * K, 15 * q + 3 * h, 3), (h * K + K - 3, 61 + 15 * q + 3 * h, 3))
            ])
            for t in (0, 1):
                cd[tile(x, t)] = dens[t]
                total = total + dens[t]
                acc = place(acc, dens[t], [
                    p for h in (0, 1) for o in (15 * q + 6 + 4 * t + 2 * h,)
                    for p in ((h * K, o, 2), (h * K + K - 2, 62 + o, 2))
                ])
        z1s[(g + 1) % G] = acc
    total = jnp.where(l8 < 2 * K, total, 0.0)

    pl.semaphore_wait(barrier, len(steps) if near else n - 1)
    first, first_y = Exchange(0), Exchange(3)

    def rim(dy, rows, skip=0):
        return part_y(dy, J - skip, rows, 0, 8 - skip - rows, skip) if not skip else (
            jnp.where(up[dy], J - skip - rows, skip), rows, jnp.where(up[dy], 8 - skip - rows, skip))

    for dy in (A, B_):
        for dx, px in groups_x():
            for dz in (1, -1):
                block(first_y, z1s, z1y, px, rim(dy, 2), (dx, dy, dz), 0, max(dz, 0))
        for count, skip in ((4, 0), (2, 1)):
            for dx, px in along_x(count, X // 2, X, 5):
                block(first_y, cp, cpy, px, rim(dy, 1, skip), (dx, dy, 0))
        for count, skip in ((5, 0), (2, 1)):
            for dx, px in along_x(count, X, 2 * X, 7):
                block(first_y, cd, cdy, px, rim(dy, 1, skip), (dx, dy, 0))
        for dz in (1, -1):
            block(first_y, z1s, z1y, (0, G, 2), rim(dy, 2), (0, dy, dz), 0, max(dz, 0))
        block(first_y, cp, cpy, (0, X, 0), rim(dy, 3), (0, dy, 0))
        block(first_y, cd, cdy, (0, 2 * X, 0), rim(dy, 2), (0, dy, 0))
    whole_rows = (0, J, 0)
    for dz in (1, -1):
        block(first, z1s, z1r, (0, G, 2), whole_rows, (0, 0, dz), 0, max(dz, 0))
        for dx, px in groups_x():
            block(first, z1s, z1r, px, whole_rows, (dx, 0, dz), 0, max(dz, 0))
    for dx, px in along_x(5, X // 2, X, 5):
        block(first, cp, cp, px, whole_rows, (dx, 0, 0))
    for dx, px in along_x(7, X, 2 * X, 7):
        block(first, cd, cd, px, whole_rows, (dx, 0, 0))

    def base(x, b):
        return 8 + ((x + 5) * 2 + b) * T

    def get(ref, x, b, off=0):
        return ref[pl.ds(base(x, b) + off, T), :]

    def own(ref, x, b, off=0):
        return ref[pl.ds(base(x, b) + H + off, J), :]

    sides = {}

    def side(x, ref, rows):
        key = (x // 4, rows)
        if key not in sides:
            sides[key] = jnp.where(lane[rows] < 60, ref[0, group(key[0])], ref[1, group(key[0])])
        return sides[key]

    def unpack(tiles, dens, zs_, rows, less, put):
        for x in range(-5, X + 5):
            far = max(-x, x - X + 1, 0) + less
            z = side(x, zs_, rows) if far < 5 else None
            if far <= 5:
                for h in (0, 1):
                    s = 15 * (x % 4) + 3 * h
                    put(B, x, h, with_sides(tiles[plane(x, 5)], h, z, K - s, 64 - s))
            for t, ref in ((0, SR), (1, SB)):
                z = side(x, zs_, rows) if far < 4 - t else None
                if far <= 4 - t:
                    for h in (0, 1):
                        s = 15 * (x % 4) + 6 + 4 * t + 2 * h
                        put(ref, x, h, with_sides(dens[tile(x, t)], h, z, K - s, 64 - s))

    def put_middle(ref, x, h, v):
        ref[pl.ds(base(x, h) + H, J), :] = v

    def put_rim(ref, x, h, v):
        ref[pl.ds(base(x, h) + H - 3, 3), :] = v[5:8]
        ref[pl.ds(base(x, h) + H + J, 3), :] = v[0:3]

    load_rw.wait()
    load_cw.wait()
    first.wait()
    unpack(cp, cd, z1r, J, 0, put_middle)
    first_y.wait()
    sides.clear()
    unpack(cpy, cdy, z1y, 8, 1, put_rim)
    sides.clear()

    sixth = jnp.float32(1.0 / 6.0)

    def beside(read, v, x, b, colour):
        c = (x + b + colour) % 2
        mid = read(v, x, b)
        t = read(v, x - 1, b) + read(v, x + 1, b)
        t = t + (read(v, x, 1 - b) + read(v, x, 1 - b, 2 * b - 1))
        return t + (mid + turn(mid, 1 - 2 * c))

    def half(depth, colour):
        new, old, src = ((R, B, SR), (B, R, SB))[colour]
        for x in range(-depth, X + depth):
            for b in (0, 1):
                new[pl.ds(base(x, b), T), :] = (beside(get, old, x, b, colour) - get(src, x, b)) * sixth

    for k in range(4):
        half(4 - k, k % 2)

    def even_at(rows):
        return (iota(rows, 0) + lane[rows]) % 2 == 0

    even = {rows: even_at(rows) for rows in {J, T}}
    one = []
    for i in range(I):
        left = None
        for x in (2 * i, 2 * i + 1):
            for b in (0, 1):
                for colour, (v, w, s) in enumerate(((R, B, SR), (B, R, SB))):
                    r = own(s, x, b) - (beside(own, w, x, b, colour) - 6.0 * own(v, x, b))
                    left = r if left is None else left + r
        one.append(left * 0.5)
    sums = [jnp.zeros((J, 128), jnp.float32) for _ in names]
    for g in range(GL):
        acc = jnp.zeros((J, 128), jnp.float32)
        for q in range(3):
            m = 3 * g + q
            red = jnp.where(even[J], one[2 * m], one[2 * m + 1])
            black = jnp.where(even[J], one[2 * m + 1], one[2 * m])
            both = two(red, black)
            if 2 * K < 128:
                both = jnp.where(l8 < 2 * K, both, 0.0)
            cl[E + m, H1 : H1 + J] = both
            sums = [a + rw[f, m] * both for f, a in enumerate(sums)]
            for c, v in enumerate((red, black)):
                s = 18 * q + 9 * c
                acc = place(acc, v, [(0, s, DEEP), (K - DEEP, 55 + s, DEEP)])
        zls[g] = acc

    def stack(rows):
        rows = [jnp.sum(v, axis=0, keepdims=True) for v in rows]
        rows = rows + [jnp.zeros((1, 128), jnp.float32)] * (Q - len(rows))
        return jnp.sum(jnp.concatenate(rows, axis=0), axis=1, keepdims=True)

    spot = lax.broadcasted_iota(jnp.int32, (Q, 128), 0) == lax.broadcasted_iota(jnp.int32, (Q, 128), 1)
    gat[0] = jnp.sum(jnp.where(spot, stack(sums + [total]), 0.0), axis=0, keepdims=True)

    def spread(o, carry):
        if isinstance(o, int):
            there = ((-(o // (ny * nz)) % nx) * ny + -(o // nz) % ny) * nz + -o % nz
        else:
            ox, oy, oz = o // (ny * nz), (o // nz) % ny, o % nz
            there = (lax.rem(nx - ox, nx) * ny + lax.rem(ny - oy, ny)) * nz + lax.rem(nz - oz, nz)
        pltpu.make_async_remote_copy(
            src_ref=gat.at[0], dst_ref=gat.at[there], send_sem=ssem.at[2], recv_sem=rsem.at[2],
            device_id=device(o), device_id_type=MESH,
        ).start()
        return carry

    def spread_y(d):
        for dx in range(nx):
            for dz in range(nz):
                if d == 0 and dx == 0 and dz == 0:
                    continue
                slot = [(-dx % nx * ny + dy % ny) * nz + -dz % nz for dy in (-abs(d), abs(d))]
                there = jnp.where(up[d], slot[0], slot[1]) if abs(d) == 1 else slot[0]
                where_y = target_y[d] if abs(d) == 1 else ys[d]
                pltpu.make_async_remote_copy(
                    src_ref=gat.at[0], dst_ref=gat.at[there], send_sem=ssem.at[2], recv_sem=rsem.at[2],
                    device_id=(xs[dx], where_y, zs[dz]), device_id_type=MESH,
                ).start()

    by_rows = n <= 64 and ny > 2
    if by_rows:
        spread_y(A)
    else:
        each_other(spread)

    second = Exchange(1)

    def deep(d, own, count, first):
        if abs(d) < 2:
            return part(d, own, min(own, count), first)
        count -= own
        return (first + own - count, count, first - own - count) if d > 0 else (first, count, first + 2 * own)

    def deep_y(d, own, count, first):
        if abs(d) < 2:
            return part_y(d, own, min(own, count), first)
        count -= own
        return part_y(d, own, count, first, first - own - count, first + 2 * own)

    def send_deep(dy):
        for dx in (1, 0) if ring else (1, -1, 0, 2, -2):
            if abs(dx) + abs(dy) > 3 or (abs(dy) == 2 and J >= DEEP) or (abs(dx) == 2 and M >= E):
                continue
            px = (0, M, M if dx else 0) if ring else deep(dx, M, E, E)
            pz = (0, GL, GL * dx) if ring else (0, GL, GL * (2 - dx))
            py = deep_y(dy, J, DEEP, H1)
            for dz in (1, -1):
                block(second, zls, zlr, pz, py, (dx, dy, dz), H1, max(dz, 0))
            if dx or dy:
                block(second, cl, cl, px, py, (dx, dy, 0))

    send_deep(A)
    if by_rows:
        for d in range(2, ny - 1):
            spread_y(d)
        spread_y(B_)
    send_deep(AA)
    send_deep(BB)
    send_deep(B_)
    send_deep(0)
    if by_rows:
        spread_y(0)

    for f in range(F):
        acc = jnp.zeros((J, 128), jnp.float32)
        for q in range(FW):
            x = f * FW + q
            v = two(own(B, x, 0), own(B, x, 1))
            cf[plane(x, 4), H : H + J] = v
            acc = place(acc, v, [
                p for h in (0, 1) for o in (4 * q + 2 * h,)
                for p in ((h * K, o, 2), (h * K + K - 2, 62 + o, 2))
            ])
        zfs[f] = acc
    fourth = Exchange(4)
    twice = nx == 2 and F == 1
    for dy in (A, B_, 0):
        for dx, px in along_x(3 if dy else 4, X // 2, X, 4):
            block(fourth, cf, cf, px, part_y(dy, J, 2, H), (dx, dy, 0))
        if dy:
            block(fourth, cf, cf, (0, X, 0), part_y(dy, J, 2, H), (0, dy, 0))
        for dx in (1, 0) if twice else (1, -1, 0):
            for dz in (1, -1):
                g0, gn, g1 = part(dx, F, 1, 1)
                block(fourth, zfs, zfr, (g0 - 1, gn, g1), part_y(dy, J, 2, H), (dx, dy, dz), H, max(dz, 0))

    others = gat.at[pl.ds(0, n - 1)]
    pltpu.make_async_copy(others, others, rsem.at[2]).wait()
    pltpu.make_async_copy(others, others, ssem.at[2]).wait()
    values = gat[:, 0, :]
    whole = jnp.sum(values, axis=0, keepdims=True)
    values = values - whole / jnp.float32(n)
    lane1 = lax.broadcasted_iota(jnp.int32, (1, 128), 1)
    cv[...] = jnp.broadcast_to(
        stack([cw[o] * values for o in range(NF)] + [jnp.where(lane1 == NF, whole, 0.0)]), (Q, 128)
    )
    mean = cv[NF : NF + 1, :] / jnp.float32(n * X * Y * Z)
    row = iota(T1, 0)
    at = lane[T1]
    maps = {}
    for dx in ((0, 1) if ring else (0, 1, -1)):
        by_row = []
        for dy in (-1, 0, 1):
            vals = [cv[names.index((dx % nx, dy % ny, dz % nz)), :][None] for dz in (-1, 0, 1)]
            by_row.append(jnp.where(at < K, vals[1], jnp.where(at < (K + 128) // 2, vals[2], vals[0])))
        field = jnp.where(row < H1, by_row[0], jnp.where(row < H1 + J, by_row[1], by_row[2]))
        maps[dx] = field + mean * jnp.float32(8.0 / 3.0)

    def base1(m):
        return 8 + ((m % (2 * M)) if ring else m + 6) * T1

    def span(depth):
        low, high = (-depth) // 2, (I - 1 + depth) // 2
        return range(2 * M) if ring and high - low + 1 >= 2 * M else range(low, high + 1)

    def window(depth):
        reach = -(-depth // 4) * 4
        return H1 - reach, J + 2 * reach

    def get1(ref, m, start, rows):
        return ref[pl.ds(base1(m) + start, rows), :]

    second.wait()
    sides.clear()
    for m in span(DEEP):
        g, q = m // 3 + (0 if ring else 2 * GL), m % 3
        if g not in sides:
            sides[g] = jnp.where(lane[T1] < 55, zlr[0, g], zlr[1, g])
        for c, ref in ((0, LR), (1, LB)):
            s = 18 * q + 9 * c
            ref[pl.ds(base1(m), T1), :] = with_sides(cl[m + E], c, sides[g], K - s, 64 - s)

    masks = {}

    def even_from(start, rows):
        if rows not in masks:
            masks[rows] = (lax.broadcasted_iota(jnp.int32, (rows, 128), 0) + lax.broadcasted_iota(jnp.int32, (rows, 128), 1)) % 2 == 0
        return masks[rows] if start % 2 == 0 else jnp.logical_not(masks[rows])

    def half1(depth, colour, shift=None, start_red=False):
        new, old, src = ((ER, EB, LR), (EB, ER, LB))[colour]
        if start_red:
            old = LR
        start, rows = window(depth)
        mask = even_from(start, rows)
        for m in span(depth):
            c = get1(old, m, start, rows)
            before, after = get1(old, m - 1, start, rows), get1(old, m + 1, start, rows)
            t = c + (jnp.where(mask, before, after) if colour == 0 else jnp.where(mask, after, before))
            t = t + (get1(old, m, start - 1, rows) + get1(old, m, start + 1, rows))
            beside_z = turn(c, 1) + turn(c, -1)
            rest = get1(src, m, start, rows) if shift is None else get1(src, m, start, rows) - shift
            t = (t + beside_z) * -sixth - rest if start_red else (t - rest) + beside_z
            new[pl.ds(base1(m) + start, rows), :] = t * sixth

    half1(8, 1, start_red=True)
    half1(7, 0)
    half1(6, 1)
    for m in span(6):
        dx = (0 if 0 <= m < M else 1) if ring else (-1 if m < 0 else (0 if m < M else 1))
        start, rows = window(6)
        EB[pl.ds(base1(m) + start, rows), :] = get1(EB, m, start, rows) + maps[dx][start : start + rows]
    shift = 4.0 * mean
    half1(5, 0, shift)
    half1(4, 1, shift)
    half1(3, 0, shift)
    half1(2, 1, shift)

    fourth.wait()
    sides.clear()
    rise = mean * jnp.float32(2.0 / 3.0)
    for m in range(-1, M + 1):
        tiles = [get1(v, m, H1 - H, T) for v in (ER, EB)]
        for i in (2 * m, 2 * m + 1):
            first_, second_ = tiles if i % 2 == 0 else tiles[::-1]
            e = jnp.where(even[T], first_, second_) + rise
            for x in (2 * i, 2 * i + 1):
                far = max(-x, x - X + 1, 0)
                z = None
                if far < 4:
                    f = 0 if x < 0 or (x >= X and twice) else (F + 1 if x >= X else x // FW + 1)
                    if f not in sides:
                        sides[f] = jnp.where(lane[T] < 60, zfr[0, f], zfr[1, f])
                    z = sides[f]
                for h in (0, 1):
                    s = 4 * (x % FW) + 2 * h
                    B[pl.ds(base(x, h), T), :] = with_sides(cf[plane(x, 4)], h, z, K - s, 64 - s) + e

    def last(depth, colour):
        new, old, src = ((R, B, SR), (B, R, SB))[colour]
        for x in range(-depth, X + depth):
            for b in (0, 1):
                t = beside(get, old, x, b, colour) - get(src, x, b) + mean
                new[pl.ds(base(x, b), T), :] = t * sixth

    last(3, 0)
    last(2, 1)
    last(1, 0)
    back = l8 >> 1
    odd_lane = (l8 & 1) == 1
    for x in range(X):
        for b in (0, 1):
            red = own(R, x, b)
            dark = (beside(own, R, x, b, 1) - own(SB, x, b) + mean) * sixth
            pair = (red, dark) if (x + b) % 2 == 0 else (dark, red)
            e, o = (jnp.take_along_axis(v, back, axis=1, mode="promise_in_bounds") for v in pair)
            out_ref[x, pl.ds(b, J, stride=2), :] = jnp.where(odd_lane, o, e)[:, 0:Z]


def body(dims, density, potential):
    nx, ny, nz, X, Y, Z = dims
    n = nx * ny * nz
    I, J, K = X // 2, Y // 2, Z // 2
    T, T1 = J + 2 * H, J + 2 * H1
    M = I // 2
    ring = nx == 2 and I < DEEP
    G, F, GL = X // 4, max(X // 12, 1), M // 3
    op = coarse_operator(nx, ny, nz, float(J * K), float(I * K), float(I * J))
    rw = residual_weights(nx, ny, nz, I, J, K)
    cw = coarse_weights(op, nx, ny, nz)
    Q = -(-(len(rw) + 1) // 8) * 8
    fine = 16 + (X + 10) * 2 * T
    coarse = 16 + (2 * M if ring else M + 12) * T1

    def vmem(*shape):
        return pltpu.VMEM(shape, jnp.float32)

    return pl.pallas_call(
        functools.partial(kernel, dims),
        out_shape=pltpu.VMEM((X, Y, Z), jnp.float32),
        in_specs=[pl.BlockSpec(memory_space=pl.ANY)] * 4,
        out_specs=pl.BlockSpec(memory_space=pltpu.VMEM),
        scratch_shapes=[
            vmem(X, Y, 128),
            vmem(X, Y, 128),
            vmem(*rw.shape),
            vmem(*cw.shape),
            vmem(X + 10, J, 128),
            vmem(X + 10, 8, 128),
            vmem(2 * X + 14, J, 128),
            vmem(2 * X + 14, 8, 128),
            vmem(X + 8, T, 128),
            vmem(2 * M if ring else M + 10, T1, 128),
            vmem(G, J, 128),
            vmem(2, G + 2, J, 128),
            vmem(2, G + 2, 8, 128),
            vmem(F, J, 128),
            vmem(2, F + 2, T, 128),
            vmem(GL, J, 128),
            vmem(2, (2 if ring else 5) * GL, T1, 128),
            vmem(fine, 128),
            vmem(fine, 128),
            vmem(fine, 128),
            vmem(fine, 128),
            vmem(coarse, 128),
            vmem(coarse, 128),
            vmem(coarse, 128),
            vmem(coarse, 128),
            vmem(n, 1, 128),
            vmem(Q, 128),
            vmem(2048, 128),
            pltpu.SemaphoreType.DMA((5,)),
            pltpu.SemaphoreType.DMA((5,)),
            pltpu.SemaphoreType.DMA((4,)),
        ],
        compiler_params=pltpu.CompilerParams(collective_id=0, has_side_effects=True),
        name="vcycle",
    )(density, potential, rw, cw)


def solution(mesh):
    nx, ny, nz = (mesh.shape[a] for a in ("gx", "gy", "gz"))

    def run(density, potential):
        return body((nx, ny, nz) + density.shape, density, potential)

    spec = P("gx", "gy", "gz")
    return jax.shard_map(run, mesh=mesh, in_specs=(spec, spec), out_specs=spec, check_vma=False)
```

```python
import functools
import numpy as np
import jax
import jax.numpy as jnp
from jax import lax
from jax.experimental import pallas as pl
from jax.experimental.pallas import tpu as pltpu
from jax.sharding import PartitionSpec as P

HI = lax.Precision.HIGHEST
MESH = pl.DeviceIdType.MESH
H, H1 = 4, 12
DEEP = 9
A, B_, AA, BB = 1, -1, 2, -2
SIDES = ((1, A), (-1, A), (0, A), (1, B_), (-1, B_), (0, B_), (0, 0), (1, 0), (-1, 0))


def table(count):
    modes = (np.arange(count) + 1) // 2
    angle = 2 * np.pi * np.outer(np.arange(count), modes) / count
    q = np.where(np.arange(count) % 2 == 1, np.cos(angle), np.sin(angle)) * np.sqrt(2 / count)
    q = np.where(2 * modes == count, np.cos(angle) / np.sqrt(count), q)
    q[:, 0] = 1 / np.sqrt(count)
    return q, 2 - 2 * np.cos(2 * np.pi * modes / count)


def coarse_operator(nx, ny, nz, wx, wy, wz):
    qx, lx = table(nx)
    qy, ly = table(ny)
    qz, lz = table(nz)
    q = np.kron(np.kron(qx, qy), qz)
    lam = wx * lx[:, None, None] + wy * ly[None, :, None] + wz * lz[None, None, :]
    lam = lam.reshape(-1)
    inv = np.concatenate([[0.0], -1.0 / lam[1:]])
    return ((q * inv) @ q.T).astype(np.float32)


def offsets(nx, ny, nz):
    steps = [(dx % nx, dy % ny, dz % nz) for dx in (0, 1, -1) for dy in (0, 1, -1) for dz in (0, 1, -1)]
    return list(dict.fromkeys(steps))


def residual_weights(nx, ny, nz, I, J, K):
    block = np.zeros((3 * I, 3 * J, 3 * K))
    block[I : 2 * I, J : 2 * J, K : 2 * K] = 1.0

    def beside(v):
        return sum(np.roll(v, d, axis) for axis in range(3) for d in (1, -1))

    red = np.indices(block.shape).sum(0) % 2 == 0
    v = beside(block) - 6.0 * block
    black2 = np.where(red, 0.0, v)
    red2 = np.where(red, v + beside(black2) / 6.0, 0.0)
    black1 = np.where(red, 0.0, beside(red2) / 6.0)
    red1 = np.where(red, beside(black1) / 6.0, 0.0)
    w = block + (black2 + red2 + black1 + red1) / 6.0
    names = offsets(nx, ny, nz)
    own = np.zeros((len(names), I, J, K))
    for dx in (0, 1, -1):
        for dy in (0, 1, -1):
            for dz in (0, 1, -1):
                x, y, z = (1 - dx) * I, (1 - dy) * J, (1 - dz) * K
                own[names.index((dx % nx, dy % ny, dz % nz))] += w[x : x + I, y : y + J, z : z + K]
    even = np.indices((J, K)).sum(0) % 2 == 0
    first, second = own[:, 0::2], own[:, 1::2]
    out = np.zeros((len(names), I // 2, J, 128))
    out[..., :K] = np.where(even, first, second)
    out[..., K : 2 * K] = np.where(even, second, first)
    return out.astype(np.float32)


def coarse_weights(op, nx, ny, nz):
    names = offsets(nx, ny, nz)
    green = op.astype(np.float64)[:, 0].reshape(nx, ny, nz)
    rx, ry, rz = np.indices((nx, ny, nz)).reshape(3, -1)
    out = np.zeros((len(names), nx * ny * nz, 128))
    for o, (ox, oy, oz) in enumerate(names):
        for f, (fx, fy, fz) in enumerate(names):
            out[o, :, f] = green[(ox - rx - fx) % nx, (oy - ry - fy) % ny, (oz - rz - fz) % nz]
    return out.astype(np.float32)


def turn(v, shift):
    shift %= 128
    return pltpu.roll(v, shift, 1) if shift else v


def kernel(
    dims, den_hbm, pot_hbm, rw_hbm, cw_hbm, out_ref,
    den_v, pot_v, rw, cw, cp, cpy, cd, cdy, cf, cl,
    z1s, z1r, z1y, zfs, zfr, zls, zlr,
    R, B, SR, SB, LR, LB, ER, EB, gat, cv, dummy,
    ssem, rsem, lsem,
):
    nx, ny, nz, X, Y, Z = dims
    n = nx * ny * nz
    I, J, K = X // 2, Y // 2, Z // 2
    T, T1 = J + 2 * H, J + 2 * H1
    M = I // 2
    ring = nx == 2 and I < DEEP
    E = 0 if ring else 5
    G, F, GL = X // 4, max(X // 12, 1), M // 3
    FW = X // F
    assert X % 12 == 0 and FW <= 12 and 2 * K <= 128 and J % 8 == 0 and 2 * J > DEEP and 2 * M >= E and M % 3 == 0
    names = offsets(nx, ny, nz)
    NF = len(names)
    Q = -(-(NF + 1) // 8) * 8
    ix, iy, iz = lax.axis_index("gx"), lax.axis_index("gy"), lax.axis_index("gz")
    me = (ix * ny + iy) * nz + iz

    def around(i, count):
        return [i] + [jnp.where(i + o >= count, i + o - count, i + o) for o in range(1, count)]

    xs, ys, zs = around(ix, nx), around(iy, ny), around(iz, nz)

    def device(o):
        if isinstance(o, int):
            return (xs[o // (ny * nz)], ys[o // nz % ny], zs[o % nz])
        ox, oy, oz = o // (ny * nz), (o // nz) % ny, o % nz
        return (lax.rem(ix + ox, nx), lax.rem(iy + oy, ny), lax.rem(iz + oz, nz))

    def each_other(step):
        if n <= 64:
            for o in range(1, n):
                step(o, 0)
        else:
            lax.fori_loop(1, n, step, 0)

    wide = (lambda ref: ref) if Z == 128 else (lambda ref: ref.at[:, :, pl.ds(0, Z)])
    load_p = pltpu.make_async_copy(pot_hbm, wide(pot_v), lsem.at[0])
    load_d = pltpu.make_async_copy(den_hbm, wide(den_v), lsem.at[1])
    load_rw = pltpu.make_async_copy(rw_hbm, rw, lsem.at[2])
    load_cw = pltpu.make_async_copy(cw_hbm, cw, lsem.at[3])

    barrier = pltpu.get_barrier_semaphore()

    def greet(o, carry):
        pl.semaphore_signal(barrier, inc=1, device_id=device(o), device_id_type=MESH)
        return carry

    near = max(nx, ny, nz) <= 5
    steps = sorted({
        (dx % nx * ny + dy % ny) * nz + dz % nz
        for dx in (-1, 0, 1) for dy in (-1, 0, 1) for dz in (-1, 0, 1)
    } - {0})
    if near:
        for o in sorted(steps, key=lambda o: o // nz % ny == 0):
            greet(o, 0)
    else:
        each_other(greet)
    load_p.start()
    load_d.start()
    load_rw.start()
    load_cw.start()

    up = {1: 2 * iy >= ny, -1: 2 * iy < ny}

    def along_y(d):
        if d == 0:
            return iy
        return jnp.where(up[1 if d > 0 else -1], ys[abs(d)], ys[-abs(d)])

    target_y = {d: along_y(d) for d in (0, 1, -1) + ((2, -2) if ny > 2 else ())}

    def part_y(d, own, count, first, low=None, high=None):
        if d == 0:
            return first, own, first
        low = first - count if low is None else low
        high = first + own if high is None else high
        goes_up = up[1 if d > 0 else -1]
        return jnp.where(goes_up, first + own - count, first), count, jnp.where(goes_up, low, high)

    class Exchange:
        def __init__(self, k):
            self.k, self.rows = k, 0

        def send(self, src, dst, at, to):
            dx, dy, dz = to
            copy = pltpu.make_async_remote_copy(
                src_ref=src, dst_ref=dst, send_sem=ssem.at[self.k], recv_sem=rsem.at[self.k],
                device_id=(xs[dx], target_y[dy], zs[dz]), device_id_type=MESH,
            )
            copy.start()
            self.rows += at

        def wait(self):
            all_of = dummy.at[pl.ds(0, self.rows)]
            pltpu.make_async_copy(all_of, all_of, rsem.at[self.k]).wait()
            pltpu.make_async_copy(all_of, all_of, ssem.at[self.k]).wait()

    def part(d, own, count, first):
        if d == 0:
            return first, own, first
        if d == 1:
            return first + own - count, count, first - count
        return first, count, first + own

    def block(ex, src, dst, px, py, to, shift=0, lead=None):
        (sx, cx, tx), (sy, cy, ty) = px, py
        target = dst if lead is None else dst.at[lead]
        ex.send(
            src.at[pl.ds(sx, cx), pl.ds(sy - shift, cy)],
            target.at[pl.ds(tx, cx), pl.ds(ty, cy)],
            cx * cy, to,
        )

    def iota(rows, dim):
        return lax.broadcasted_iota(jnp.int32, (rows, 128), dim)

    lane = {rows: iota(rows, 1) for rows in {8, J, T, T1}}

    def place(acc, v, pieces):
        by_shift = {}
        for src, dst, width in pieces:
            by_shift.setdefault((dst - src) % 128, []).append((dst, width))
        at = lane[v.shape[0]]
        for shift, spans in by_shift.items():
            mask = None
            for dst, width in spans:
                inside = (at >= dst) & (at < dst + width)
                mask = inside if mask is None else mask | inside
            moved = turn(v, shift)
            acc = jnp.where(mask, moved, acc)
        return acc

    def outside(z, right, left):
        if (right - left) % 128 == 0:
            return turn(z, right)
        return jnp.where(lane[z.shape[0]] < 96, turn(z, right), turn(z, left))

    def with_sides(v, half, z, right, left):
        own = turn(v, -K) if half else v
        if z is None:
            return own
        return jnp.where(lane[v.shape[0]] < K, own, outside(z, right, left))

    def two(a, b):
        return jnp.where(lane[a.shape[0]] < K, a, turn(b, K))

    l8 = lane[J]
    low = jnp.where(l8 < K, 2 * l8, 2 * (l8 - K) + 1) & 127
    high = jnp.where(l8 < K, 2 * l8 + 1, 2 * (l8 - K)) & 127
    order = (low, high)

    def colours(ref, x, which):
        v = [ref[x, pl.ds(b, J, stride=2), :] for b in (0, 1)]
        take = [jnp.take_along_axis(u, order[which], axis=1, mode="promise_in_bounds") for u in v]
        return jnp.where(l8 < K, take[0], take[1])

    def plane(x, deep):
        if 0 <= x < X:
            return (x + X // 2) % X
        return X + deep + x if x < 0 else deep + x

    def tile(x, t):
        if 0 <= x < X:
            return 2 * plane(x, 4) + (t if x < X // 2 else 1 - t)
        return 2 * X + (6 + 2 * (x + 1) - t if x < 0 else 7 + 2 * (x - X) + t)

    def group(g):
        return 0 if g < 0 else (1 if g >= G else 2 + (g + 1) % G)

    def along_x(count, middle, halo, halo_size):
        if nx == 2:
            return [(1, (middle - count, 2 * count, halo + halo_size - count))]
        return [(1, (middle - count, count, halo + halo_size - count)), (-1, (middle, count, halo + halo_size))]

    def groups_x():
        return [(1, (0, 2, 0))] if nx == 2 else [(1, (0, 1, 0)), (-1, (1, 1, 1))]

    load_p.wait()
    load_d.wait()
    total = jnp.zeros((J, 128), jnp.float32)
    for g in range(G):
        acc = jnp.zeros((J, 128), jnp.float32)
        for q in range(4):
            x = 4 * g + q
            black = colours(pot_v, x, 1 - x % 2)
            dens = [colours(den_v, x, x % 2), colours(den_v, x, 1 - x % 2)]
            cp[plane(x, 5)] = black
            acc = place(acc, black, [
                p for h in (0, 1)
                for p in ((h * K, 15 * q + 3 * h, 3), (h * K + K - 3, 61 + 15 * q + 3 * h, 3))
            ])
            for t in (0, 1):
                cd[tile(x, t)] = dens[t]
                total = total + dens[t]
                acc = place(acc, dens[t], [
                    p for h in (0, 1) for o in (15 * q + 6 + 4 * t + 2 * h,)
                    for p in ((h * K, o, 2), (h * K + K - 2, 62 + o, 2))
                ])
        z1s[(g + 1) % G] = acc
    total = jnp.where(l8 < 2 * K, total, 0.0)

    pl.semaphore_wait(barrier, len(steps) if near else n - 1)
    first, first_y = Exchange(0), Exchange(3)

    def rim(dy, rows, skip=0):
        return part_y(dy, J - skip, rows, 0, 8 - skip - rows, skip) if not skip else (
            jnp.where(up[dy], J - skip - rows, skip), rows, jnp.where(up[dy], 8 - skip - rows, skip))

    for dy in (A, B_):
        for dx, px in groups_x():
            for dz in (1, -1):
                block(first_y, z1s, z1y, px, rim(dy, 2), (dx, dy, dz), 0, max(dz, 0))
        for count, skip in ((4, 0), (2, 1)):
            for dx, px in along_x(count, X // 2, X, 5):
                block(first_y, cp, cpy, px, rim(dy, 1, skip), (dx, dy, 0))
        for count, skip in ((5, 0), (2, 1)):
            for dx, px in along_x(count, X, 2 * X, 7):
                block(first_y, cd, cdy, px, rim(dy, 1, skip), (dx, dy, 0))
        for dz in (1, -1):
            block(first_y, z1s, z1y, (0, G, 2), rim(dy, 2), (0, dy, dz), 0, max(dz, 0))
        block(first_y, cp, cpy, (0, X, 0), rim(dy, 3), (0, dy, 0))
        block(first_y, cd, cdy, (0, 2 * X, 0), rim(dy, 2), (0, dy, 0))
    whole_rows = (0, J, 0)
    for dz in (1, -1):
        block(first, z1s, z1r, (0, G, 2), whole_rows, (0, 0, dz), 0, max(dz, 0))
        for dx, px in groups_x():
            block(first, z1s, z1r, px, whole_rows, (dx, 0, dz), 0, max(dz, 0))
    for dx, px in along_x(5, X // 2, X, 5):
        block(first, cp, cp, px, whole_rows, (dx, 0, 0))
    for dx, px in along_x(7, X, 2 * X, 7):
        block(first, cd, cd, px, whole_rows, (dx, 0, 0))

    def base(x, b):
        return 8 + ((x + 5) * 2 + b) * T

    def get(ref, x, b, off=0):
        return ref[pl.ds(base(x, b) + off, T), :]

    def own(ref, x, b, off=0):
        return ref[pl.ds(base(x, b) + H + off, J), :]

    sides = {}

    def side(x, ref, rows):
        key = (x // 4, rows)
        if key not in sides:
            sides[key] = jnp.where(lane[rows] < 60, ref[0, group(key[0])], ref[1, group(key[0])])
        return sides[key]

    def unpack(tiles, dens, zs_, rows, less, put):
        for x in range(-5, X + 5):
            far = max(-x, x - X + 1, 0) + less
            z = side(x, zs_, rows) if far < 5 else None
            if far <= 5:
                for h in (0, 1):
                    s = 15 * (x % 4) + 3 * h
                    put(B, x, h, with_sides(tiles[plane(x, 5)], h, z, K - s, 64 - s))
            for t, ref in ((0, SR), (1, SB)):
                z = side(x, zs_, rows) if far < 4 - t else None
                if far <= 4 - t:
                    for h in (0, 1):
                        s = 15 * (x % 4) + 6 + 4 * t + 2 * h
                        put(ref, x, h, with_sides(dens[tile(x, t)], h, z, K - s, 64 - s))

    def put_middle(ref, x, h, v):
        ref[pl.ds(base(x, h) + H, J), :] = v

    def put_rim(ref, x, h, v):
        ref[pl.ds(base(x, h) + H - 3, 3), :] = v[5:8]
        ref[pl.ds(base(x, h) + H + J, 3), :] = v[0:3]

    load_rw.wait()
    load_cw.wait()
    first.wait()
    unpack(cp, cd, z1r, J, 0, put_middle)
    first_y.wait()
    sides.clear()
    unpack(cpy, cdy, z1y, 8, 1, put_rim)
    sides.clear()

    sixth = jnp.float32(1.0 / 6.0)

    def beside(read, v, x, b, colour):
        c = (x + b + colour) % 2
        mid = read(v, x, b)
        t = read(v, x - 1, b) + read(v, x + 1, b)
        t = t + (read(v, x, 1 - b) + read(v, x, 1 - b, 2 * b - 1))
        return t + (mid + turn(mid, 1 - 2 * c))

    def half(depth, colour):
        new, old, src = ((R, B, SR), (B, R, SB))[colour]
        for x in range(-depth, X + depth):
            for b in (0, 1):
                new[pl.ds(base(x, b), T), :] = (beside(get, old, x, b, colour) - get(src, x, b)) * sixth

    for k in range(4):
        half(4 - k, k % 2)

    def even_at(rows):
        return (iota(rows, 0) + lane[rows]) % 2 == 0

    even = {rows: even_at(rows) for rows in {J, T}}
    one = []
    for i in range(I):
        left = None
        for x in (2 * i, 2 * i + 1):
            for b in (0, 1):
                for colour, (v, w, s) in enumerate(((R, B, SR), (B, R, SB))):
                    r = own(s, x, b) - (beside(own, w, x, b, colour) - 6.0 * own(v, x, b))
                    left = r if left is None else left + r
        one.append(left * 0.5)
    sums = [jnp.zeros((J, 128), jnp.float32) for _ in names]
    for g in range(GL):
        acc = jnp.zeros((J, 128), jnp.float32)
        for q in range(3):
            m = 3 * g + q
            red = jnp.where(even[J], one[2 * m], one[2 * m + 1])
            black = jnp.where(even[J], one[2 * m + 1], one[2 * m])
            both = two(red, black)
            if 2 * K < 128:
                both = jnp.where(l8 < 2 * K, both, 0.0)
            cl[E + m, H1 : H1 + J] = both
            sums = [a + rw[f, m] * both for f, a in enumerate(sums)]
            for c, v in enumerate((red, black)):
                s = 18 * q + 9 * c
                acc = place(acc, v, [(0, s, DEEP), (K - DEEP, 55 + s, DEEP)])
        zls[g] = acc

    def stack(rows):
        rows = [jnp.sum(v, axis=0, keepdims=True) for v in rows]
        rows = rows + [jnp.zeros((1, 128), jnp.float32)] * (Q - len(rows))
        return jnp.sum(jnp.concatenate(rows, axis=0), axis=1, keepdims=True)

    spot = lax.broadcasted_iota(jnp.int32, (Q, 128), 0) == lax.broadcasted_iota(jnp.int32, (Q, 128), 1)
    gat[0] = jnp.sum(jnp.where(spot, stack(sums + [total]), 0.0), axis=0, keepdims=True)

    def spread(o, carry):
        if isinstance(o, int):
            there = ((-(o // (ny * nz)) % nx) * ny + -(o // nz) % ny) * nz + -o % nz
        else:
            ox, oy, oz = o // (ny * nz), (o // nz) % ny, o % nz
            there = (lax.rem(nx - ox, nx) * ny + lax.rem(ny - oy, ny)) * nz + lax.rem(nz - oz, nz)
        pltpu.make_async_remote_copy(
            src_ref=gat.at[0], dst_ref=gat.at[there], send_sem=ssem.at[2], recv_sem=rsem.at[2],
            device_id=device(o), device_id_type=MESH,
        ).start()
        return carry

    def spread_y(d):
        for dx in range(nx):
            for dz in range(nz):
                if d == 0 and dx == 0 and dz == 0:
                    continue
                slot = [(-dx % nx * ny + dy % ny) * nz + -dz % nz for dy in (-abs(d), abs(d))]
                there = jnp.where(up[d], slot[0], slot[1]) if abs(d) == 1 else slot[0]
                where_y = target_y[d] if abs(d) == 1 else ys[d]
                pltpu.make_async_remote_copy(
                    src_ref=gat.at[0], dst_ref=gat.at[there], send_sem=ssem.at[2], recv_sem=rsem.at[2],
                    device_id=(xs[dx], where_y, zs[dz]), device_id_type=MESH,
                ).start()

    by_rows = n <= 64 and ny > 2
    if by_rows:
        spread_y(A)
    else:
        each_other(spread)

    second = Exchange(1)

    def deep(d, own, count, first):
        if abs(d) < 2:
            return part(d, own, min(own, count), first)
        count -= own
        return (first + own - count, count, first - own - count) if d > 0 else (first, count, first + 2 * own)

    def deep_y(d, own, count, first):
        if abs(d) < 2:
            return part_y(d, own, min(own, count), first)
        count -= own
        return part_y(d, own, count, first, first - own - count, first + 2 * own)

    def send_deep(dy):
        for dx in (1, 0) if ring else (1, -1, 0, 2, -2):
            if abs(dx) + abs(dy) > 3 or (abs(dy) == 2 and J >= DEEP) or (abs(dx) == 2 and M >= E):
                continue
            px = (0, M, M if dx else 0) if ring else deep(dx, M, E, E)
            pz = (0, GL, GL * dx) if ring else (0, GL, GL * (2 - dx))
            py = deep_y(dy, J, DEEP, H1)
            for dz in (1, -1):
                block(second, zls, zlr, pz, py, (dx, dy, dz), H1, max(dz, 0))
            if dx or dy:
                block(second, cl, cl, px, py, (dx, dy, 0))

    send_deep(A)
    if by_rows:
        for d in range(2, ny - 1):
            spread_y(d)
        spread_y(B_)
    send_deep(AA)
    send_deep(BB)
    send_deep(B_)
    send_deep(0)
    if by_rows:
        spread_y(0)

    for f in range(F):
        acc = jnp.zeros((J, 128), jnp.float32)
        for q in range(FW):
            x = f * FW + q
            v = two(own(B, x, 0), own(B, x, 1))
            cf[plane(x, 4), H : H + J] = v
            acc = place(acc, v, [
                p for h in (0, 1) for o in (4 * q + 2 * h,)
                for p in ((h * K, o, 2), (h * K + K - 2, 62 + o, 2))
            ])
        zfs[f] = acc
    fourth = Exchange(4)
    twice = nx == 2 and F == 1
    for dy in (A, B_, 0):
        for count, row in ((3, 0), (1, 1)) if dy else ((4, 0),):
            for dx, px in along_x(count, X // 2, X, 4):
                py = part_y(dy, J, J, H)
                if dy:
                    py = (jnp.where(up[dy], H + J - 1 - row, H + row), 1, jnp.where(up[dy], H - 1 - row, H + J + row))
                block(fourth, cf, cf, px, py, (dx, dy, 0))
        if dy:
            block(fourth, cf, cf, (0, X, 0), part_y(dy, J, 2, H), (0, dy, 0))
        for dx in (1, 0) if twice else (1, -1, 0):
            for dz in (1, -1):
                g0, gn, g1 = part(dx, F, 1, 1)
                block(fourth, zfs, zfr, (g0 - 1, gn, g1), part_y(dy, J, 2, H), (dx, dy, dz), H, max(dz, 0))

    others = gat.at[pl.ds(0, n - 1)]
    pltpu.make_async_copy(others, others, rsem.at[2]).wait()
    pltpu.make_async_copy(others, others, ssem.at[2]).wait()
    values = gat[:, 0, :]
    whole = jnp.sum(values, axis=0, keepdims=True)
    values = values - whole / jnp.float32(n)
    lane1 = lax.broadcasted_iota(jnp.int32, (1, 128), 1)
    cv[...] = jnp.broadcast_to(
        stack([cw[o] * values for o in range(NF)] + [jnp.where(lane1 == NF, whole, 0.0)]), (Q, 128)
    )
    mean = cv[NF : NF + 1, :] / jnp.float32(n * X * Y * Z)
    row = iota(T1, 0)
    at = lane[T1]
    maps = {}
    for dx in ((0, 1) if ring else (0, 1, -1)):
        by_row = []
        for dy in (-1, 0, 1):
            vals = [cv[names.index((dx % nx, dy % ny, dz % nz)), :][None] for dz in (-1, 0, 1)]
            by_row.append(jnp.where(at < K, vals[1], jnp.where(at < (K + 128) // 2, vals[2], vals[0])))
        field = jnp.where(row < H1, by_row[0], jnp.where(row < H1 + J, by_row[1], by_row[2]))
        maps[dx] = field + mean * jnp.float32(8.0 / 3.0)

    def base1(m):
        return 8 + ((m % (2 * M)) if ring else m + 6) * T1

    def span(depth):
        low, high = (-depth) // 2, (I - 1 + depth) // 2
        return range(2 * M) if ring and high - low + 1 >= 2 * M else range(low, high + 1)

    def window(depth):
        reach = -(-depth // 4) * 4
        return H1 - reach, J + 2 * reach

    def get1(ref, m, start, rows):
        return ref[pl.ds(base1(m) + start, rows), :]

    second.wait()
    sides.clear()
    for m in span(DEEP):
        g, q = m // 3 + (0 if ring else 2 * GL), m % 3
        if g not in sides:
            sides[g] = jnp.where(lane[T1] < 55, zlr[0, g], zlr[1, g])
        for c, ref in ((0, LR), (1, LB)):
            s = 18 * q + 9 * c
            ref[pl.ds(base1(m), T1), :] = with_sides(cl[m + E], c, sides[g], K - s, 64 - s)

    masks = {}

    def even_from(start, rows):
        if rows not in masks:
            masks[rows] = (lax.broadcasted_iota(jnp.int32, (rows, 128), 0) + lax.broadcasted_iota(jnp.int32, (rows, 128), 1)) % 2 == 0
        return masks[rows] if start % 2 == 0 else jnp.logical_not(masks[rows])

    def half1(depth, colour, shift=None, start_red=False):
        new, old, src = ((ER, EB, LR), (EB, ER, LB))[colour]
        if start_red:
            old = LR
        start, rows = window(depth)
        mask = even_from(start, rows)
        for m in span(depth):
            c = get1(old, m, start, rows)
            before, after = get1(old, m - 1, start, rows), get1(old, m + 1, start, rows)
            t = c + (jnp.where(mask, before, after) if colour == 0 else jnp.where(mask, after, before))
            t = t + (get1(old, m, start - 1, rows) + get1(old, m, start + 1, rows))
            beside_z = turn(c, 1) + turn(c, -1)
            rest = get1(src, m, start, rows) if shift is None else get1(src, m, start, rows) - shift
            t = (t + beside_z) * -sixth - rest if start_red else (t - rest) + beside_z
            new[pl.ds(base1(m) + start, rows), :] = t * sixth

    half1(8, 1, start_red=True)
    half1(7, 0)
    half1(6, 1)
    for m in span(6):
        dx = (0 if 0 <= m < M else 1) if ring else (-1 if m < 0 else (0 if m < M else 1))
        start, rows = window(6)
        EB[pl.ds(base1(m) + start, rows), :] = get1(EB, m, start, rows) + maps[dx][start : start + rows]
    shift = 4.0 * mean
    half1(5, 0, shift)
    half1(4, 1, shift)
    half1(3, 0, shift)
    half1(2, 1, shift)

    fourth.wait()
    sides.clear()
    rise = mean * jnp.float32(2.0 / 3.0)
    for m in range(-1, M + 1):
        tiles = [get1(v, m, H1 - H, T) for v in (ER, EB)]
        for i in (2 * m, 2 * m + 1):
            first_, second_ = tiles if i % 2 == 0 else tiles[::-1]
            e = jnp.where(even[T], first_, second_) + rise
            for x in (2 * i, 2 * i + 1):
                far = max(-x, x - X + 1, 0)
                z = None
                if far < 4:
                    f = 0 if x < 0 or (x >= X and twice) else (F + 1 if x >= X else x // FW + 1)
                    if f not in sides:
                        sides[f] = jnp.where(lane[T] < 60, zfr[0, f], zfr[1, f])
                    z = sides[f]
                for h in (0, 1):
                    s = 4 * (x % FW) + 2 * h
                    B[pl.ds(base(x, h), T), :] = with_sides(cf[plane(x, 4)], h, z, K - s, 64 - s) + e

    def last(depth, colour):
        new, old, src = ((R, B, SR), (B, R, SB))[colour]
        for x in range(-depth, X + depth):
            for b in (0, 1):
                t = beside(get, old, x, b, colour) - get(src, x, b) + mean
                new[pl.ds(base(x, b), T), :] = t * sixth

    last(3, 0)
    last(2, 1)
    last(1, 0)
    back = l8 >> 1
    odd_lane = (l8 & 1) == 1
    for x in range(X):
        for b in (0, 1):
            red = own(R, x, b)
            dark = (beside(own, R, x, b, 1) - own(SB, x, b) + mean) * sixth
            pair = (red, dark) if (x + b) % 2 == 0 else (dark, red)
            e, o = (jnp.take_along_axis(v, back, axis=1, mode="promise_in_bounds") for v in pair)
            out_ref[x, pl.ds(b, J, stride=2), :] = jnp.where(odd_lane, o, e)[:, 0:Z]


def body(dims, density, potential):
    nx, ny, nz, X, Y, Z = dims
    n = nx * ny * nz
    I, J, K = X // 2, Y // 2, Z // 2
    T, T1 = J + 2 * H, J + 2 * H1
    M = I // 2
    ring = nx == 2 and I < DEEP
    G, F, GL = X // 4, max(X // 12, 1), M // 3
    op = coarse_operator(nx, ny, nz, float(J * K), float(I * K), float(I * J))
    rw = residual_weights(nx, ny, nz, I, J, K)
    cw = coarse_weights(op, nx, ny, nz)
    Q = -(-(len(rw) + 1) // 8) * 8
    fine = 16 + (X + 10) * 2 * T
    coarse = 16 + (2 * M if ring else M + 12) * T1

    def vmem(*shape):
        return pltpu.VMEM(shape, jnp.float32)

    return pl.pallas_call(
        functools.partial(kernel, dims),
        out_shape=pltpu.VMEM((X, Y, Z), jnp.float32),
        in_specs=[pl.BlockSpec(memory_space=pl.ANY)] * 4,
        out_specs=pl.BlockSpec(memory_space=pltpu.VMEM),
        scratch_shapes=[
            vmem(X, Y, 128),
            vmem(X, Y, 128),
            vmem(*rw.shape),
            vmem(*cw.shape),
            vmem(X + 10, J, 128),
            vmem(X + 10, 8, 128),
            vmem(2 * X + 14, J, 128),
            vmem(2 * X + 14, 8, 128),
            vmem(X + 8, T, 128),
            vmem(2 * M if ring else M + 10, T1, 128),
            vmem(G, J, 128),
            vmem(2, G + 2, J, 128),
            vmem(2, G + 2, 8, 128),
            vmem(F, J, 128),
            vmem(2, F + 2, T, 128),
            vmem(GL, J, 128),
            vmem(2, (2 if ring else 5) * GL, T1, 128),
            vmem(fine, 128),
            vmem(fine, 128),
            vmem(fine, 128),
            vmem(fine, 128),
            vmem(coarse, 128),
            vmem(coarse, 128),
            vmem(coarse, 128),
            vmem(coarse, 128),
            vmem(n, 1, 128),
            vmem(Q, 128),
            vmem(2048, 128),
            pltpu.SemaphoreType.DMA((5,)),
            pltpu.SemaphoreType.DMA((5,)),
            pltpu.SemaphoreType.DMA((4,)),
        ],
        compiler_params=pltpu.CompilerParams(collective_id=0, has_side_effects=True),
        name="vcycle",
    )(density, potential, rw, cw)


def solution(mesh):
    nx, ny, nz = (mesh.shape[a] for a in ("gx", "gy", "gz"))

    def run(density, potential):
        return body((nx, ny, nz) + density.shape, density, potential)

    spec = P("gx", "gy", "gz")
    return jax.shard_map(run, mesh=mesh, in_specs=(spec, spec), out_specs=spec, check_vma=False)
```
